32 devices in a mesh: grp: 2 (over x), blk: 8 (over z, y), vec: 2 (over core).
Axes of the slice: x: 2, y: 2, z: 4, core: 2. Of those that a mesh axis runs over, the one named last changes fastest.
Arguments:
- trial: bfloat16 [20480, 32], P(('grp', 'blk', 'vec')), may hold values from -6 to 6
- energy_gap: float32 [20480], P(('grp', 'blk', 'vec')), may hold values from 0.5 to 2.5
- coulomb_factors: bfloat16 [4096, 20480], P('blk'), may hold values from -0.0390625 to 0.0390625
- occ_values: bfloat16 [80, 40, 512], P('blk'), may hold values from -1 to 1
- vir_values: bfloat16 [80, 512, 512], P('blk'), may hold values from -1 to 1
- kernel: float32 [80, 512], P('blk'), may hold values from 0.2 to 2
- live_points: int32 [80], P('blk'), may hold values from 64 to 512
Outputs:
- sigma: bfloat16 [20480, 32], P(('grp', 'blk', 'vec'))
The draws below stay inside these ranges and needn't reach their ends.
All inputs are finite; a program needn't handle non-finite values.
Results may differ from the reference program's by a relative error of at most 0.0029.
Values may be sent and summed in bfloat16 or wider, within the bound.
No kernel may reach another device: no remote copies, remote signals or barrier semaphores. Data moves between devices by JAX's collectives and lax.ppermute only.
A program may use at most 64 MiB of HBM per device.

```python
import math
import jax
import jax.numpy as jnp
from jax import lax

NOCC = 40
NVIR = 512
NAUX = 4096
K = 32
BATCH = 512
BATCHES = 80
POINTS = 40960
PAIRS = 20480


def touch_ends(values, stream_key, smallest, top_value):
    place = [jax.random.randint(jax.random.fold_in(stream_key, axis), (), 0, length) for axis, length in enumerate(values.shape)]
    widest = values.shape.index(max(values.shape))
    next_to = place[:widest] + [(place[widest] + 1) % values.shape[widest]] + place[widest + 1:]
    return values.at[tuple(place)].set(smallest).at[tuple(next_to)].set(top_value)


def steps_of(own_key, shape, split, smallest, top_value):
    gain, own = 1.0, jax.random.fold_in(own_key, 6)
    for dim, parts in split:
        heights = jnp.exp(jax.random.uniform(jax.random.fold_in(own, dim), (parts,), jnp.float32, smallest / len(split), top_value / len(split)))
        gain = gain * jnp.repeat(heights, shape[dim] // parts).reshape([-1 if axis == dim else 1 for axis in range(len(shape))])
    return gain


def centred(stream_key, dims, spread, reach, shards=(), kind=jnp.bfloat16):
    values = jax.random.normal(stream_key, dims, jnp.float32) * spread
    if len(shards) > 0:
        values = steps_of(stream_key, dims, shards, -0.22, 0.18) * values
    return jnp.clip(values, min=-reach, max=reach).astype(kind)


def setup_inputs(seed: int = 0) -> dict:
    keys = jax.random.split(jax.random.key(seed), 8)
    trial = centred(keys[0], (PAIRS, K), 1.0, 6.0, ((0, 32),))
    energy_gap = jnp.clip(0.5 + 2.0 * jax.random.uniform(keys[1], (PAIRS,), jnp.float32) ** steps_of(keys[1], (PAIRS,), ((0, 32),), -0.2, 0.2), 0.5, 2.5)
    coulomb_factors = centred(keys[2], (NAUX, PAIRS), (NAUX + PAIRS) ** -0.5, 0.0390625, ((0, 8),))
    occ_values = centred(keys[3], (BATCHES, NOCC, BATCH), ((POINTS * PAIRS) ** -0.125), 1.0, ((0, 8),))
    vir_values = centred(keys[4], (BATCHES, BATCH, NVIR), ((POINTS * PAIRS) ** -0.125), 1.0, ((0, 8),))
    kernel = jnp.clip(jnp.exp(math.log(2.0) - 2.3025851 * jax.random.uniform(keys[5], (BATCHES, BATCH), jnp.float32) ** steps_of(keys[5], (BATCHES, BATCH), ((0, 8),), -0.2, 0.2)), 0.2, 2.0)
    live_points = touch_ends(jax.random.randint(keys[6], (BATCHES,), BATCH // 8, BATCH + 1), jax.random.fold_in(keys[6], 1), BATCH // 8, BATCH).astype(jnp.int32)
    return {"trial": trial, "energy_gap": energy_gap, "coulomb_factors": coulomb_factors, "occ_values": occ_values, "vir_values": vir_values, "kernel": kernel, "live_points": live_points}


def reference(trial, energy_gap, coulomb_factors, occ_values, vir_values, kernel, live_points):
    factored = jnp.dot(coulomb_factors, trial, preferred_element_type=jnp.float32).astype(jnp.bfloat16)
    coulomb = 2.0 * lax.dot_general(coulomb_factors, factored, (((0,), (0,)), ((), ())), preferred_element_type=jnp.float32)
    width = trial.shape[1]
    rearranged = trial.reshape(NOCC, NVIR, width).transpose(1, 0, 2).reshape(NVIR, NOCC * width)
    slots = jnp.arange(BATCH, dtype=jnp.int32)

    def step(carry, items):
        occ, vir, weight, live = items
        trans = jnp.dot(vir, rearranged, preferred_element_type=jnp.float32).reshape(BATCH, NOCC, width)
        occ_float = occ.astype(jnp.float32)
        density = jnp.einsum("gik,ig->gk", trans, occ_float)
        mask = (slots < live).astype(jnp.float32)
        weighted = density * (weight * mask)[:, None]
        scaled = (occ_float.T[:, :, None] * weighted[:, None, :]).reshape(BATCH, NOCC * width).astype(jnp.bfloat16)
        return carry + lax.dot_general(vir, scaled, (((0,), (0,)), ((), ())), preferred_element_type=jnp.float32), None

    start = jnp.zeros((NVIR, NOCC * width), jnp.float32)
    total, _ = lax.scan(step, start, (occ_values, vir_values, kernel, live_points))
    exchange = total.reshape(NVIR, NOCC, width).transpose(1, 0, 2).reshape(NOCC * NVIR, width)
    result = energy_gap[:, None] * trial.astype(jnp.float32) + coulomb + exchange
    return result.astype(jnp.bfloat16)
```

```python
import jax
import jax.numpy as jnp
from jax import lax
from jax.experimental import pallas as pl
from jax.experimental.pallas import tpu as pltpu
from jax.sharding import PartitionSpec as P

LANES = 128
NT = (((1,), (1,)), ((), ()))
NN = (((1,), (0,)), ((), ()))


def digits_of(count):
    digits, stride = [], 1
    bits = count.bit_length() - 1
    if bits % 2:
        digits.append((1, 2))
        stride = 2
    while stride < count:
        digits.append((stride, 4))
        stride *= 4
    return digits


def swap(x, axis, count, mask):
    return lax.ppermute(x, axis, [(i, i ^ mask) for i in range(count)])


def first_kernel(half, masks, *refs):
    pieces = refs[: len(masks)]
    occ_ref, vir_hbm, fac_hbm, dens_ref, part_ref, rows, flat, occ32, vir, fac, vsem, fsem = refs[
        len(masks) :
    ]
    me, grp = lax.axis_index("blk"), lax.axis_index("grp")
    batches, points, virs = vir_hbm.shape
    occs = rows.shape[0] // half
    chunks = fac.shape[0]
    wide = fac.shape[2]
    start = pl.multiple_of(grp * (occs * virs), LANES)

    def vir_copy(b):
        return pltpu.make_async_copy(vir_hbm.at[b], vir.at[b], vsem.at[b])

    def fac_copy(c):
        at = pl.multiple_of(start + c * wide, LANES)
        return pltpu.make_async_copy(fac_hbm.at[:, pl.ds(at, wide)], fac.at[c], fsem.at[c])

    for n in range(max(batches, chunks)):
        if n < batches:
            vir_copy(n).start()
        if n < chunks:
            fac_copy(n).start()

    tiles = virs // LANES
    for piece, mask in zip(pieces, masks):
        parts, _, length = piece.shape
        per = length // LANES
        for p in range(parts):
            for j in range(per):
                at = (me ^ mask) * (parts * per) + p * per + j if len(masks) > 1 else p * per + j
                block = piece[p, :, j * LANES : (j + 1) * LANES]
                i, t = at // tiles, at % tiles
                rows[
                    pl.ds(pl.multiple_of(i * half, half), half),
                    pl.ds(pl.multiple_of(t * LANES, LANES), LANES),
                ] = block
                flat[:, pl.ds(pl.multiple_of(at * LANES, LANES), LANES)] = block

    def dens_step(b, _):
        vir_copy(b).wait()
        occ32[...] = occ_ref[b].astype(jnp.float32)
        trans = lax.dot_general(rows[...], vir[b], NT, preferred_element_type=jnp.float32)
        total = jnp.zeros((half, points), jnp.float32)
        for i in range(occs):
            row = occ32[pl.ds(grp * occs + i, 1), :]
            total = total + row * trans[i * half : (i + 1) * half, :]
        dens_ref[b] = total.astype(dens_ref.dtype)
        return 0

    lax.fori_loop(0, batches, dens_step, 0)

    part_ref[...] = jnp.zeros(part_ref.shape, jnp.float32)

    def fac_step(c, _):
        fac_copy(c).wait()
        x = flat[:, pl.ds(pl.multiple_of(c * wide, LANES), wide)]
        part_ref[...] += lax.dot_general(x, fac[c], NT, preferred_element_type=jnp.float32)
        return 0

    lax.fori_loop(0, chunks, fac_step, 0)


def second_kernel(half, blocks, *refs):
    (
        live_ref, dens_a, dens_b, part_a, part_b, occ_ref, weight_ref, vir_hbm, fac_hbm,
    ) = refs[:9]
    outs = refs[9:-9]
    occ32, vir, fac, vsem, fsem, scaled, acc, both, held = refs[-9:]
    me, grp = lax.axis_index("blk"), lax.axis_index("grp")
    batches, points, virs = vir_hbm.shape
    occs = scaled.shape[0] // half
    chunks = fac.shape[0]
    wide = fac.shape[2]
    start = pl.multiple_of(grp * (occs * virs), LANES)

    def vir_copy(b):
        return pltpu.make_async_copy(vir_hbm.at[b], vir.at[b], vsem.at[b])

    def fac_copy(c):
        at = pl.multiple_of(start + c * wide, LANES)
        return pltpu.make_async_copy(fac_hbm.at[:, pl.ds(at, wide)], fac.at[c], fsem.at[c])

    for n in range(max(batches, chunks)):
        if n < batches:
            vir_copy(n).start()
        if n < chunks:
            fac_copy(n).start()

    slots = lax.broadcasted_iota(jnp.int32, (1, points), 1)
    acc[...] = jnp.zeros(acc.shape, jnp.float32)

    def grid_step(b, _):
        vir_copy(b).wait()
        occ32[...] = occ_ref[b].astype(jnp.float32)
        density = dens_a[b].astype(jnp.float32) + dens_b[b].astype(jnp.float32)
        weight = jnp.where(slots < live_ref[b], weight_ref[pl.ds(b, 1), :], 0.0)
        weighted = density * weight
        for i in range(occs):
            row = occ32[pl.ds(grp * occs + i, 1), :]
            scaled[i * half : (i + 1) * half, :] = (row * weighted).astype(jnp.bfloat16)
        acc[...] += lax.dot_general(scaled[...], vir[b], NN, preferred_element_type=jnp.float32)
        return 0

    lax.fori_loop(0, batches, grid_step, 0)

    both[...] = (part_a[...] + part_b[...]).astype(jnp.bfloat16)
    count, parts, length = blocks
    per = length // LANES
    tiles = virs // LANES
    each = wide // LANES

    def fac_step(c, _):
        fac_copy(c).wait()
        coulomb = 2.0 * lax.dot_general(both[...], fac[c], NN, preferred_element_type=jnp.float32)
        for t in range(each):
            at = c * each + t
            i, lane = at // tiles, at % tiles
            value = coulomb[:, t * LANES : (t + 1) * LANES] + acc[
                pl.ds(pl.multiple_of(i * half, half), half),
                pl.ds(pl.multiple_of(lane * LANES, LANES), LANES),
            ]
            owner, rest = at // (parts * per), at % (parts * per)
            slot = owner ^ me if count > 1 else owner
            held[
                slot, rest // per, :, pl.ds(pl.multiple_of((rest % per) * LANES, LANES), LANES)
            ] = value
        return 0

    lax.fori_loop(0, chunks, fac_step, 0)

    radix = len(outs)
    for d, out in enumerate(outs):
        for n in range(out.shape[0]):
            out[n] = held[n * radix + d].astype(out.dtype)


def local(trial, energy_gap, coulomb_factors, occ_values, vir_values, kernel, live_points, sizes):
    groups, blks, vecs = sizes
    rows, k = trial.shape
    half = k // vecs
    aux, pairs = coulomb_factors.shape
    batches, occ_count, points = occ_values.shape
    virs = vir_values.shape[2]
    mine = pairs // groups
    occs = occ_count // groups
    digits = digits_of(blks)
    vec = lax.axis_index("vec")
    me = lax.axis_index("blk")
    vmem = pl.BlockSpec(memory_space=pltpu.VMEM)
    anywhere = pl.BlockSpec(memory_space=pl.ANY)

    wide_rows = trial.T.reshape(vecs, half, rows)
    keep = lax.dynamic_index_in_dim(wide_rows, vec, 0, keepdims=False)
    give = lax.dynamic_index_in_dim(wide_rows, 1 - vec, 0, keepdims=False)
    take = swap(give, "vec", vecs, 1)
    first = vec == 0
    own = jnp.stack([jnp.where(first, keep, take), jnp.where(first, take, keep)])

    pieces, masks = [own], [0]
    for stride, radix in reversed(digits):
        base_pieces, base_masks = list(pieces), list(masks)
        for d in range(1, radix):
            for piece, mask in zip(base_pieces, base_masks):
                pieces.append(swap(piece, "blk", blks, d * stride))
                masks.append(mask ^ (d * stride))

    aligned = rows % LANES == 0
    if not aligned:
        ordered = jnp.stack([p for _, p in sorted(zip(masks, pieces), key=lambda x: x[0])])
        ordered = jnp.take(ordered, me ^ jnp.arange(blks), axis=0)
        pieces = [ordered.transpose(2, 0, 1, 3).reshape(1, half, mine)]
        masks = [0]

    chunks = 5 if (mine // LANES) % 5 == 0 else 1
    wide = mine // chunks
    scratch = [
        pltpu.VMEM((occ_count, points), jnp.float32),
        pltpu.VMEM((batches, points, virs), jnp.bfloat16),
        pltpu.VMEM((chunks, aux, wide), jnp.bfloat16),
        pltpu.SemaphoreType.DMA((batches,)),
        pltpu.SemaphoreType.DMA((chunks,)),
    ]
    limit = pltpu.CompilerParams(vmem_limit_bytes=40 * 2**20)
    dens, part = pl.pallas_call(
        lambda *refs: first_kernel(half, tuple(masks), *refs),
        out_shape=(
            jax.ShapeDtypeStruct((batches, half, points), jnp.float32),
            jax.ShapeDtypeStruct((half, aux), jnp.float32),
        ),
        in_specs=[vmem] * len(pieces) + [vmem, anywhere, anywhere],
        out_specs=(vmem, vmem),
        scratch_shapes=[
            pltpu.VMEM((occs * half, virs), jnp.bfloat16),
            pltpu.VMEM((half, mine), jnp.bfloat16),
        ]
        + scratch,
        compiler_params=limit,
        name="first",
        cost_estimate=pl.CostEstimate(
            flops=2 * half * mine * (aux + batches * points),
            bytes_accessed=2 * (aux * mine + vir_values.size),
            transcendentals=0,
        ),
    )(*pieces, occ_values, vir_values, coulomb_factors)

    other_part = swap(part, "grp", groups, 1)
    other_dens = swap(dens.astype(jnp.bfloat16), "grp", groups, 1)

    if aligned:
        blocks = (blks, vecs, rows)
        radix = digits[0][1]
    else:
        blocks = (1, 1, mine)
        radix = 1
    held = (blocks[0], blocks[1], half, blocks[2])
    out_shape = tuple(
        jax.ShapeDtypeStruct(
            (blocks[0] // radix,) + held[1:], jnp.float32 if d == 0 else jnp.bfloat16
        )
        for d in range(radix)
    )
    sums = pl.pallas_call(
        lambda *refs: second_kernel(half, blocks, *refs),
        out_shape=out_shape,
        in_specs=[pl.BlockSpec(memory_space=pltpu.SMEM)] + [vmem] * 6 + [anywhere, anywhere],
        out_specs=tuple(vmem for _ in out_shape),
        scratch_shapes=scratch
        + [
            pltpu.VMEM((occs * half, points), jnp.bfloat16),
            pltpu.VMEM((occs * half, virs), jnp.float32),
            pltpu.VMEM((half, aux), jnp.bfloat16),
            pltpu.VMEM(held, jnp.float32),
        ],
        compiler_params=limit,
        name="second",
        cost_estimate=pl.CostEstimate(
            flops=2 * half * mine * (aux + batches * points),
            bytes_accessed=2 * (aux * mine + vir_values.size),
            transcendentals=0,
        ),
    )(live_points, dens, other_dens, part, other_part, occ_values, kernel, vir_values, coulomb_factors)

    if aligned:
        stay, sends = sums[0], list(sums[1:])
    else:
        full = sums[0].reshape(half, blks, vecs, rows).transpose(1, 2, 0, 3)
        full = jnp.take(full, me ^ jnp.arange(blks), axis=0)
        radix = digits[0][1]
        full = full.reshape((blks // radix, radix) + full.shape[1:])
        stay = full[:, 0]
        sends = [full[:, d].astype(jnp.bfloat16) for d in range(1, radix)]

    for level, (stride, radix) in enumerate(digits):
        total = stay
        for d in range(1, radix):
            total = total + swap(sends[d - 1], "blk", blks, d * stride).astype(jnp.float32)
        if level + 1 < len(digits):
            radix = digits[level + 1][1]
            total = total.reshape((-1, radix) + total.shape[1:])
            stay = total[:, 0]
            sends = [total[:, d].astype(jnp.bfloat16) for d in range(1, radix)]
    total = total.reshape(vecs, half, rows)

    keep = lax.dynamic_index_in_dim(total, vec, 0, keepdims=False)
    give = lax.dynamic_index_in_dim(total, 1 - vec, 0, keepdims=False)
    take = swap(give, "vec", vecs, 1)
    joined = jnp.concatenate([jnp.where(first, keep, take), jnp.where(first, take, keep)])
    result = energy_gap[None, :] * trial.T.astype(jnp.float32) + joined
    return result.astype(jnp.bfloat16).T


def solution(mesh):
    sizes = tuple(mesh.shape[a] for a in ("grp", "blk", "vec"))
    in_specs = (
        P(("grp", "blk", "vec"), None),
        P(("grp", "blk", "vec")),
        P("blk", None),
        P("blk", None, None),
        P("blk", None, None),
        P("blk", None),
        P("blk"),
    )
    out_specs = P(("grp", "blk", "vec"), None)

    def program(*args):
        return local(*args, sizes=sizes)

    return jax.shard_map(program, mesh=mesh, in_specs=in_specs, out_specs=out_specs, check_vma=False)
```

```python
import jax
import jax.numpy as jnp
from jax import lax
from jax.experimental import pallas as pl
from jax.experimental.pallas import tpu as pltpu
from jax.sharding import PartitionSpec as P

LANES = 128
NT = (((1,), (1,)), ((), ()))
NN = (((1,), (0,)), ((), ()))
VMEM = pl.BlockSpec(memory_space=pltpu.VMEM)
SMEM = pl.BlockSpec(memory_space=pltpu.SMEM)
HBM = pl.BlockSpec(memory_space=pltpu.HBM)


def digits_of(count):
    digits, stride = [], 1
    bits = count.bit_length() - 1
    if bits % 2:
        digits.append((1, 2))
        stride = 2
    while stride < count:
        digits.append((stride, 4))
        stride *= 4
    return digits


def swap(x, axis, count, mask):
    return lax.ppermute(x, axis, [(i, i ^ mask) for i in range(count)])


def call(body, out_shape, in_specs, flops=0, scratch=(), limit=24, name=None):
    return pl.pallas_call(
        body,
        out_shape=out_shape,
        in_specs=in_specs,
        out_specs=jax.tree.map(lambda _: VMEM, out_shape),
        scratch_shapes=list(scratch),
        compiler_params=pltpu.CompilerParams(vmem_limit_bytes=limit * 2**20),
        name=name,
        cost_estimate=pl.CostEstimate(flops=flops, bytes_accessed=0, transcendentals=0),
    )


def shape(dims, dtype):
    return jax.ShapeDtypeStruct(dims, dtype)


class Plan:
    def __init__(self, sizes, trial, coulomb_factors, occ_values, vir_values):
        self.groups, self.blks, self.vecs = sizes
        self.rows, self.k = trial.shape
        self.aux = coulomb_factors.shape[0] // self.vecs
        self.pairs = coulomb_factors.shape[1] // self.groups
        self.batches = occ_values.shape[0] // self.vecs
        self.occ_all, self.points = occ_values.shape[1:]
        self.occs = self.occ_all // self.groups
        self.virs = vir_values.shape[2]
        self.aligned = self.rows % LANES == 0
        self.count = self.blks if self.aligned else 1
        self.length = self.rows if self.aligned else self.pairs // self.vecs
        self.per = self.length // LANES

    def owner(self, m):
        return lax.axis_index("blk") ^ m if self.aligned else 0

    def part(self, h):
        return lax.axis_index("vec") ^ h if self.aligned else h

    def block(self, h, m, j):
        return (self.owner(m) * self.vecs + self.part(h)) * self.per + j

    def place(self, h, m, j):
        at = self.block(h, m, j)
        tiles = self.virs // LANES
        return (
            pl.ds(pl.multiple_of((at // tiles) * self.k, self.k), self.k),
            pl.ds(pl.multiple_of((at % tiles) * LANES, LANES), LANES),
        )


def load_kernel(plan, fac_hbm, vir_hbm, occ_hbm, fac, vir, occ, occ_in, fsem, vsem, osem):
    grp, vec = lax.axis_index("grp"), lax.axis_index("vec")
    top = pl.multiple_of(vec * plan.aux, 8)
    base = vec * plan.batches
    copies = [
        pltpu.make_async_copy(occ_hbm.at[pl.ds(base, plan.batches)], occ_in, osem),
        pltpu.make_async_copy(vir_hbm.at[pl.ds(base, plan.batches)], vir, vsem),
    ]
    for h in range(plan.vecs):
        for m in range(plan.count):
            at = pl.multiple_of(grp * plan.pairs + plan.block(h, m, 0) * LANES, LANES)
            copies.append(
                pltpu.make_async_copy(
                    fac_hbm.at[pl.ds(top, plan.aux), pl.ds(at, plan.length)],
                    fac.at[h, :, pl.ds(m * plan.length, plan.length)],
                    fsem.at[h, m],
                )
            )
    for copy in copies:
        copy.start()
    copies[0].wait()
    for b in range(plan.batches):
        value = occ_in[b].astype(jnp.float32)
        chosen = value[: plan.occs]
        for q in range(1, plan.groups):
            chosen = jnp.where(grp == q, value[q * plan.occs : (q + 1) * plan.occs], chosen)
        occ[b] = chosen
    for copy in copies[1:]:
        copy.wait()


def flat_of(ref, count):
    return jnp.concatenate([ref[m] for m in range(count)], axis=1)


def stack_kernel(plan, *refs):
    for m, piece in enumerate(refs[1:-1]):
        refs[-1][m] = piece[...]


def fac_kernel(plan, h, half, fac, *refs):
    value = lax.dot_general(
        flat_of(half, plan.count), fac[h], NT, preferred_element_type=jnp.float32
    )
    if len(refs) > 1:
        value = value + refs[0][...]
    refs[-1][...] = value


def dens_kernel(plan, mine, other, vir, occ, dens, sent, rows):
    k = plan.k
    for h, half in enumerate((mine, other)):
        for m in range(plan.count):
            for j in range(plan.per):
                rows[plan.place(h, m, j)] = half[m, :, j * LANES : (j + 1) * LANES]
    for b in range(plan.batches):
        trans = lax.dot_general(rows[...], vir[b], NT, preferred_element_type=jnp.float32)
        total = occ[b, 0:1, :] * trans[:k, :]
        for i in range(1, plan.occs):
            total = total + occ[b, i : i + 1, :] * trans[i * k : (i + 1) * k, :]
        dens[b] = total
        sent[b] = total.astype(sent.dtype)


def back_kernel(plan, part_a, part_b, fac, out):
    both = (part_a[...] + part_b[...]).astype(jnp.bfloat16)
    for h in range(plan.vecs):
        value = 2.0 * lax.dot_general(both, fac[h], NN, preferred_element_type=jnp.float32)
        for m in range(plan.count):
            out[h, m] = value[:, m * plan.length : (m + 1) * plan.length]


def grid_kernel(plan, live, dens_a, dens_b, occ, weight, vir, coulomb, stay, sent, scaled, acc):
    k = plan.k
    base = lax.axis_index("vec") * plan.batches
    slots = lax.broadcasted_iota(jnp.int32, (1, plan.points), 1)
    for b in range(plan.batches):
        density = dens_a[b] + dens_b[b].astype(jnp.float32)
        used = jnp.where(slots < live[base + b], weight[pl.ds(base + b, 1), :], 0.0)
        weighted = density * used
        for i in range(plan.occs):
            scaled[i * k : (i + 1) * k, :] = (occ[b, i : i + 1, :] * weighted).astype(jnp.bfloat16)
        value = lax.dot_general(scaled[...], vir[b], NN, preferred_element_type=jnp.float32)
        if b == 0:
            acc[...] = value
        else:
            acc[...] += value
    for h, out in enumerate((stay, sent)):
        for m in range(plan.count):
            for j in range(plan.per):
                lanes = slice(j * LANES, (j + 1) * LANES)
                value = coulomb[h, m, :, lanes] + acc[plan.place(h, m, j)]
                out[m, :, lanes] = value.astype(out.dtype)


def local(trial, energy_gap, coulomb_factors, occ_values, vir_values, kernel, live_points, sizes):
    plan = Plan(sizes, trial, coulomb_factors, occ_values, vir_values)
    groups, blks, vecs, k = plan.groups, plan.blks, plan.vecs, plan.k
    batches, points, virs, occs = plan.batches, plan.points, plan.virs, plan.occs
    digits = digits_of(blks)
    half = (plan.count, k, plan.length)
    bf16, f32 = jnp.bfloat16, jnp.float32

    def bind(body, *first):
        return lambda *refs: body(plan, *first, *refs)

    fac, vir, occ = call(
        bind(load_kernel),
        (
            shape((vecs, plan.aux, plan.count * plan.length), bf16),
            shape((batches, points, virs), bf16),
            shape((batches, occs, points), f32),
        ),
        [HBM] * 3,
        flops=10**9,
        scratch=[
            pltpu.VMEM((batches, plan.occ_all, points), bf16),
            pltpu.SemaphoreType.DMA((vecs, plan.count)),
            pltpu.SemaphoreType.DMA,
            pltpu.SemaphoreType.DMA,
        ],
        limit=44,
        name="load",
    )(coulomb_factors, vir_values, occ_values)

    pieces, masks = [trial.T], [0]
    for stride, radix in reversed(digits):
        known = len(masks)
        for d in range(1, radix):
            for n in range(known):
                pieces.append(swap(pieces[n], "blk", blks, d * stride))
                masks.append(masks[n] ^ (d * stride))
    pieces = [p for _, p in sorted(zip(masks, pieces), key=lambda pair: pair[0])]

    if plan.aligned:
        mine = call(
            bind(stack_kernel), shape(half, bf16), [VMEM] * (len(pieces) + 1), name="stack"
        )(occ, *pieces)
        other = swap(mine, "vec", vecs, 1)
    else:
        me, vec = lax.axis_index("blk"), lax.axis_index("vec")
        mine = jnp.take(jnp.stack(pieces), me ^ jnp.arange(blks), axis=0)
        both = jnp.stack([mine, swap(mine, "vec", vecs, 1)])
        both = jnp.take(both, vec ^ jnp.arange(vecs), axis=0)
        both = both.transpose(2, 1, 0, 3).reshape(k, vecs, plan.length)
        mine, other = both[None, :, 0], both[None, :, 1]

    flops = 2 * k * plan.aux * plan.pairs // 2
    part = call(bind(fac_kernel, 0), shape((k, plan.aux), f32), [VMEM] * 2, flops, name="fac0")(
        mine, fac
    )
    part = call(bind(fac_kernel, 1), shape((k, plan.aux), f32), [VMEM] * 3, flops, name="fac1")(
        other, fac, part
    )
    other_part = swap(part, "grp", groups, 1)

    grid_flops = 2 * batches * points * virs * occs * k
    dens, sent = call(
        bind(dens_kernel),
        (shape((batches, k, points), f32), shape((batches, k, points), bf16)),
        [VMEM] * 4,
        grid_flops,
        [pltpu.VMEM((occs * k, virs), bf16)],
        name="dens",
    )(mine, other, vir, occ)
    other_dens = swap(sent, "grp", groups, 1)

    coulomb = call(
        bind(back_kernel), shape((vecs,) + half, f32), [VMEM] * 3, 2 * flops, name="back"
    )(part, other_part, fac)
    stay, sent = call(
        bind(grid_kernel),
        (shape(half, f32), shape(half, bf16)),
        [SMEM] + [VMEM] * 6,
        grid_flops,
        [pltpu.VMEM((occs * k, points), bf16), pltpu.VMEM((occs * k, virs), f32)],
        name="grid",
    )(live_points, dens, other_dens, occ, kernel, vir, coulomb)

    if plan.aligned:
        total = stay + swap(sent, "vec", vecs, 1).astype(f32)
    else:
        full = jnp.concatenate([stay[0], sent[0].astype(f32)], axis=1)
        full = full.reshape(k, blks, vecs, plan.rows).transpose(2, 1, 0, 3)
        full = jnp.take(full, me ^ jnp.arange(blks), axis=1)
        full = jnp.take(full, vec ^ jnp.arange(vecs), axis=0)
        total = full[0] + swap(full[1].astype(bf16), "vec", vecs, 1).astype(f32)

    for stride, radix in digits:
        total = total.reshape((-1, radix) + total.shape[1:])
        came = [
            swap(total[:, d].astype(bf16), "blk", blks, d * stride).astype(f32)
            for d in range(1, radix)
        ]
        total = sum(came, total[:, 0])
    result = energy_gap[None, :] * trial.T.astype(f32) + total[0]
    return result.astype(bf16).T


def solution(mesh):
    sizes = tuple(mesh.shape[a] for a in ("grp", "blk", "vec"))
    in_specs = (
        P(("grp", "blk", "vec"), None),
        P(("grp", "blk", "vec")),
        P("blk", None),
        P("blk", None, None),
        P("blk", None, None),
        P("blk", None),
        P("blk"),
    )
    out_specs = P(("grp", "blk", "vec"), None)

    def program(*args):
        return local(*args, sizes=sizes)

    return jax.shard_map(program, mesh=mesh, in_specs=in_specs, out_specs=out_specs, check_vma=False)
```

```python
import jax
import jax.numpy as jnp
from jax import lax
from jax.experimental import pallas as pl
from jax.experimental.pallas import tpu as pltpu
from jax.sharding import PartitionSpec as P

LANES = 128
HEAD = 10**10
NT = (((1,), (1,)), ((), ()))
NN = (((1,), (0,)), ((), ()))
VMEM = pl.BlockSpec(memory_space=pltpu.VMEM)
SMEM = pl.BlockSpec(memory_space=pltpu.SMEM)
HBM = pl.BlockSpec(memory_space=pltpu.HBM)


def digits_of(count):
    digits, stride = [], 1
    bits = count.bit_length() - 1
    if bits % 2:
        digits.append((1, 2))
        stride = 2
    while stride < count:
        digits.append((stride, 4))
        stride *= 4
    return digits


def swap(x, axis, count, mask):
    return lax.ppermute(x, axis, [(i, i ^ mask) for i in range(count)])


def call(body, out_shape, in_specs, flops=0, scratch=(), limit=24, name=None):
    return pl.pallas_call(
        body,
        out_shape=out_shape,
        in_specs=in_specs,
        out_specs=jax.tree.map(lambda _: VMEM, out_shape),
        scratch_shapes=list(scratch),
        compiler_params=pltpu.CompilerParams(vmem_limit_bytes=limit * 2**20),
        name=name,
        cost_estimate=pl.CostEstimate(flops=flops, bytes_accessed=0, transcendentals=0),
    )


def shape(dims, dtype):
    return jax.ShapeDtypeStruct(dims, dtype)


class Plan:
    def __init__(self, sizes, trial, coulomb_factors, occ_values, vir_values):
        self.groups, self.blks, self.vecs = sizes
        self.rows, self.k = trial.shape
        self.aux = coulomb_factors.shape[0] // self.vecs
        self.pairs = coulomb_factors.shape[1] // self.groups
        self.batches = occ_values.shape[0] // self.vecs
        self.occ_all, self.points = occ_values.shape[1:]
        self.occs = self.occ_all // self.groups
        self.virs = vir_values.shape[2]
        self.aligned = self.rows % LANES == 0
        self.count = self.blks if self.aligned else 1
        self.length = self.rows if self.aligned else self.pairs // self.vecs
        self.per = self.length // LANES

    def owner(self, m):
        return lax.axis_index("blk") ^ m if self.aligned else 0

    def part(self, h):
        return lax.axis_index("vec") ^ h if self.aligned else h

    def block(self, h, m, j):
        return (self.owner(m) * self.vecs + self.part(h)) * self.per + j

    def place(self, h, m, j):
        at = self.block(h, m, j)
        tiles = self.virs // LANES
        return (
            pl.ds(pl.multiple_of((at // tiles) * self.k, self.k), self.k),
            pl.ds(pl.multiple_of((at % tiles) * LANES, LANES), LANES),
        )


def head_kernel(plan, given, out):
    out[...] = given[...]


def flat_of(ref, count):
    return jnp.concatenate([ref[m] for m in range(count)], axis=1)


def stack_kernel(plan, *refs):
    for m, piece in enumerate(refs[:-1]):
        refs[-1][m] = piece[...]


def occ_rows(plan, occ, b, occ32):
    occ32[...] = occ[lax.axis_index("vec") * plan.batches + b].astype(jnp.float32)
    base = lax.axis_index("grp") * plan.occs
    return lambda i: occ32[pl.ds(base + i, 1), :]


def dens_kernel(plan, mine, other, vir, occ, fac_hbm, dens, sent, fac, rows, occ32, fsem):
    k = plan.k
    grp, vec = lax.axis_index("grp"), lax.axis_index("vec")
    top = pl.multiple_of(vec * plan.aux, 8)
    copies = []
    for h in range(plan.vecs):
        for m in range(plan.count):
            at = pl.multiple_of(grp * plan.pairs + plan.block(h, m, 0) * LANES, LANES)
            copies.append(
                pltpu.make_async_copy(
                    fac_hbm.at[pl.ds(top, plan.aux), pl.ds(at, plan.length)],
                    fac.at[h, :, pl.ds(m * plan.length, plan.length)],
                    fsem.at[h, m],
                )
            )
    for copy in copies:
        copy.start()
    for h, half in enumerate((mine, other)):
        for m in range(plan.count):
            for j in range(plan.per):
                rows[plan.place(h, m, j)] = half[m, :, j * LANES : (j + 1) * LANES]
    for b in range(plan.batches):
        row = occ_rows(plan, occ, b, occ32.at[b])
        trans = lax.dot_general(
            rows[...], vir[vec * plan.batches + b], NT, preferred_element_type=jnp.float32
        )
        total = row(0) * trans[:k, :]
        for i in range(1, plan.occs):
            total = total + row(i) * trans[i * k : (i + 1) * k, :]
        dens[b] = total
        sent[b] = total.astype(sent.dtype)
    for copy in copies:
        copy.wait()


def fac_kernel(plan, mine, other, fac, out):
    value = 0.0
    for h, half in enumerate((mine, other)):
        value += lax.dot_general(
            flat_of(half, plan.count), fac[h], NT, preferred_element_type=jnp.float32
        )
    out[...] = value


def grid_kernel(plan, live, dens_a, dens_b, occ, weight, vir, acc, scaled, occ32):
    k = plan.k
    base = lax.axis_index("vec") * plan.batches
    slots = lax.broadcasted_iota(jnp.int32, (1, plan.points), 1)
    for b in range(plan.batches):
        row = occ_rows(plan, occ, b, occ32.at[b])
        density = dens_a[b] + dens_b[b].astype(jnp.float32)
        used = jnp.where(slots < live[base + b], weight[pl.ds(base + b, 1), :], 0.0)
        weighted = density * used
        for i in range(plan.occs):
            scaled[i * k : (i + 1) * k, :] = (row(i) * weighted).astype(jnp.bfloat16)
        value = lax.dot_general(
            scaled[...], vir[base + b], NN, preferred_element_type=jnp.float32
        )
        if b == 0:
            acc[...] = value
        else:
            acc[...] += value


def back_kernel(plan, part_a, part_b, fac, acc, stay, sent):
    both = (part_a[...] + part_b[...]).astype(jnp.bfloat16)
    for h, out in enumerate((stay, sent)):
        value = 2.0 * lax.dot_general(both, fac[h], NN, preferred_element_type=jnp.float32)
        for m in range(plan.count):
            for j in range(plan.per):
                at = m * plan.length + j * LANES
                total = value[:, at : at + LANES] + acc[plan.place(h, m, j)]
                out[m, :, j * LANES : (j + 1) * LANES] = total.astype(out.dtype)


def local(trial, energy_gap, coulomb_factors, occ_values, vir_values, kernel, live_points, sizes):
    plan = Plan(sizes, trial, coulomb_factors, occ_values, vir_values)
    groups, blks, vecs, k = plan.groups, plan.blks, plan.vecs, plan.k
    batches, points, virs, occs = plan.batches, plan.points, plan.virs, plan.occs
    digits = digits_of(blks)
    half = (plan.count, k, plan.length)
    bf16, f32 = jnp.bfloat16, jnp.float32

    def bind(body, *first):
        return lambda *refs: body(plan, *first, *refs)

    trial_cols = trial.T
    start = call(
        bind(head_kernel), shape(trial_cols.shape, bf16), [VMEM], flops=HEAD, name="head"
    )(trial_cols)
    pieces, masks = [start], [0]
    for stride, radix in reversed(digits):
        known = len(masks)
        for d in range(1, radix):
            for n in range(known):
                pieces.append(swap(pieces[n], "blk", blks, d * stride))
                masks.append(masks[n] ^ (d * stride))
    pieces = [p for _, p in sorted(zip(masks, pieces), key=lambda pair: pair[0])]

    if plan.aligned:
        mine = call(bind(stack_kernel), shape(half, bf16), [VMEM] * len(pieces), name="stack")(
            *pieces
        )
        other = swap(mine, "vec", vecs, 1)
    else:
        me, vec = lax.axis_index("blk"), lax.axis_index("vec")
        mine = jnp.take(jnp.stack(pieces), me ^ jnp.arange(blks), axis=0)
        both = jnp.stack([mine, swap(mine, "vec", vecs, 1)])
        both = jnp.take(both, vec ^ jnp.arange(vecs), axis=0)
        both = both.transpose(2, 1, 0, 3).reshape(k, vecs, plan.length)
        mine, other = both[None, :, 0], both[None, :, 1]

    flops = 2 * k * plan.aux * plan.pairs
    grid_flops = 2 * batches * points * virs * occs * k
    occ_scratch = pltpu.VMEM((batches, plan.occ_all, points), f32)
    dens, sent, fac = call(
        bind(dens_kernel),
        (
            shape((batches, k, points), f32),
            shape((batches, k, points), bf16),
            shape((vecs, plan.aux, plan.count * plan.length), bf16),
        ),
        [VMEM] * 4 + [HBM],
        grid_flops,
        [
            pltpu.VMEM((occs * k, virs), bf16),
            occ_scratch,
            pltpu.SemaphoreType.DMA((vecs, plan.count)),
        ],
        name="dens",
    )(mine, other, vir_values, occ_values, coulomb_factors)
    other_dens = swap(sent, "grp", groups, 1)

    part = call(bind(fac_kernel), shape((k, plan.aux), f32), [VMEM] * 3, flops, name="fac")(
        mine, other, fac
    )
    other_part = swap(part, "grp", groups, 1)

    acc = call(
        bind(grid_kernel),
        shape((occs * k, virs), f32),
        [SMEM] + [VMEM] * 5,
        grid_flops,
        [pltpu.VMEM((occs * k, points), bf16), occ_scratch],
        name="grid",
    )(live_points, dens, other_dens, occ_values, kernel, vir_values)
    stay, sent = call(
        bind(back_kernel), (shape(half, f32), shape(half, bf16)), [VMEM] * 4, flops, name="back"
    )(part, other_part, fac, acc)

    if plan.aligned:
        total = stay + swap(sent, "vec", vecs, 1).astype(f32)
    else:
        full = jnp.concatenate([stay[0], sent[0].astype(f32)], axis=1)
        full = full.reshape(k, blks, vecs, plan.rows).transpose(2, 1, 0, 3)
        full = jnp.take(full, me ^ jnp.arange(blks), axis=1)
        full = jnp.take(full, vec ^ jnp.arange(vecs), axis=0)
        total = full[0] + swap(full[1].astype(bf16), "vec", vecs, 1).astype(f32)

    for stride, radix in digits:
        total = total.reshape((-1, radix) + total.shape[1:])
        came = [
            swap(total[:, d].astype(bf16), "blk", blks, d * stride).astype(f32)
            for d in range(1, radix)
        ]
        total = sum(came, total[:, 0])
    result = energy_gap[None, :] * start.astype(f32) + total[0]
    return result.astype(bf16).T


def solution(mesh):
    sizes = tuple(mesh.shape[a] for a in ("grp", "blk", "vec"))
    in_specs = (
        P(("grp", "blk", "vec"), None),
        P(("grp", "blk", "vec")),
        P("blk", None),
        P("blk", None, None),
        P("blk", None, None),
        P("blk", None),
        P("blk"),
    )
    out_specs = P(("grp", "blk", "vec"), None)

    def program(*args):
        return local(*args, sizes=sizes)

    return jax.shard_map(program, mesh=mesh, in_specs=in_specs, out_specs=out_specs, check_vma=False)
```

```python
import jax
import jax.numpy as jnp
from jax import lax
from jax.experimental import pallas as pl
from jax.experimental.pallas import tpu as pltpu
from jax.sharding import PartitionSpec as P

LANES = 128
HEAD = 10**10
NT = (((1,), (1,)), ((), ()))
NN = (((1,), (0,)), ((), ()))
VMEM = pl.BlockSpec(memory_space=pltpu.VMEM)
SMEM = pl.BlockSpec(memory_space=pltpu.SMEM)
HBM = pl.BlockSpec(memory_space=pltpu.HBM)


def digits_of(count):
    digits, stride = [], 1
    bits = count.bit_length() - 1
    if bits % 2:
        digits.append((1, 2))
        stride = 2
    while stride < count:
        digits.append((stride, 4))
        stride *= 4
    return digits


def swap(x, axis, count, mask):
    return lax.ppermute(x, axis, [(i, i ^ mask) for i in range(count)])


def call(body, out_shape, in_specs, flops=0, scratch=(), limit=14, name=None):
    return pl.pallas_call(
        body,
        out_shape=out_shape,
        in_specs=in_specs,
        out_specs=jax.tree.map(lambda _: VMEM, out_shape),
        scratch_shapes=list(scratch),
        compiler_params=pltpu.CompilerParams(vmem_limit_bytes=limit * 2**20),
        name=name,
        cost_estimate=pl.CostEstimate(flops=flops, bytes_accessed=0, transcendentals=0),
    )


def shape(dims, dtype):
    return jax.ShapeDtypeStruct(dims, dtype)


class Plan:
    def __init__(self, sizes, trial, coulomb_factors, occ_values, vir_values):
        self.groups, self.blks, self.vecs = sizes
        self.rows, self.k = trial.shape
        self.aux = coulomb_factors.shape[0] // self.vecs
        self.pairs = coulomb_factors.shape[1] // self.groups
        self.batches = occ_values.shape[0] // self.vecs
        self.occ_all, self.points = occ_values.shape[1:]
        self.occs = self.occ_all // self.groups
        self.virs = vir_values.shape[2]
        self.aligned = self.rows % LANES == 0
        self.count = self.blks if self.aligned else 1
        self.length = self.rows if self.aligned else self.pairs // self.vecs
        self.per = self.length // LANES

    def owner(self, m):
        return lax.axis_index("blk") ^ m if self.aligned else 0

    def part(self, h):
        return lax.axis_index("vec") ^ h if self.aligned else h

    def block(self, h, m, j):
        return (self.owner(m) * self.vecs + self.part(h)) * self.per + j

    def place(self, h, m, j):
        at = self.block(h, m, j)
        tiles = self.virs // LANES
        return (
            pl.ds(pl.multiple_of((at // tiles) * self.k, self.k), self.k),
            pl.ds(pl.multiple_of((at % tiles) * LANES, LANES), LANES),
        )


def head_kernel(plan, given, out):
    out[...] = given[...]


def stack_kernel(plan, *refs):
    for m, piece in enumerate(refs[:-1]):
        refs[-1][m] = piece[...]


def occ_rows(plan, occ, b, occ32):
    occ32[...] = occ[lax.axis_index("vec") * plan.batches + b].astype(jnp.float32)
    base = lax.axis_index("grp") * plan.occs
    return lambda i: occ32[pl.ds(base + i, 1), :]


def factor_block(plan, fac, m, width):
    top = pl.multiple_of(lax.axis_index("vec") * plan.aux, plan.aux)
    at = lax.axis_index("grp") * plan.pairs + plan.owner(m) * width
    return fac[pl.ds(top, plan.aux), pl.ds(pl.multiple_of(at, LANES), width)]


def dens_kernel(plan, mine, other, vir, occ, dens, sent, rows, occ32):
    k = plan.k
    vec = lax.axis_index("vec")
    for h, half in enumerate((mine, other)):
        for m in range(plan.count):
            for j in range(plan.per):
                rows[plan.place(h, m, j)] = half[m, :, j * LANES : (j + 1) * LANES]
    for b in range(plan.batches):
        row = occ_rows(plan, occ, b, occ32.at[b])
        trans = lax.dot_general(
            rows[...], vir[vec * plan.batches + b], NT, preferred_element_type=jnp.float32
        )
        total = row(0) * trans[:k, :]
        for i in range(1, plan.occs):
            total = total + row(i) * trans[i * k : (i + 1) * k, :]
        dens[b] = total
        sent[b] = total.astype(sent.dtype)


def fac_kernel(plan, mine, other, fac, out, flat):
    width = plan.vecs * plan.length
    for h, half in enumerate((mine, other)):
        for m in range(plan.count):
            at = m * width + plan.part(h) * plan.length
            flat[:, pl.ds(pl.multiple_of(at, LANES), plan.length)] = half[m]
    value = 0.0
    for m in range(plan.count):
        value += lax.dot_general(
            flat[:, m * width : (m + 1) * width],
            factor_block(plan, fac, m, width),
            NT,
            preferred_element_type=jnp.float32,
        )
    out[...] = value


def grid_kernel(plan, live, dens_a, dens_b, occ, weight, vir, acc, scaled, occ32):
    k = plan.k
    base = lax.axis_index("vec") * plan.batches
    slots = lax.broadcasted_iota(jnp.int32, (1, plan.points), 1)
    for b in range(plan.batches):
        row = occ_rows(plan, occ, b, occ32.at[b])
        density = dens_a[b] + dens_b[b].astype(jnp.float32)
        used = jnp.where(slots < live[base + b], weight[pl.ds(base + b, 1), :], 0.0)
        weighted = density * used
        for i in range(plan.occs):
            scaled[i * k : (i + 1) * k, :] = (row(i) * weighted).astype(jnp.bfloat16)
        value = lax.dot_general(
            scaled[...], vir[base + b], NN, preferred_element_type=jnp.float32
        )
        if b == 0:
            acc[...] = value
        else:
            acc[...] += value


def back_kernel(plan, part_a, part_b, fac, acc, stay, sent):
    both = (part_a[...] + part_b[...]).astype(jnp.bfloat16)
    width = plan.vecs * plan.length
    for m in range(plan.count):
        value = 2.0 * lax.dot_general(
            both, factor_block(plan, fac, m, width), NN, preferred_element_type=jnp.float32
        )
        for h, out in enumerate((stay, sent)):
            chosen = value[:, : plan.length]
            for p in range(1, plan.vecs):
                part = value[:, p * plan.length : (p + 1) * plan.length]
                chosen = jnp.where(plan.part(h) == p, part, chosen)
            for j in range(plan.per):
                lanes = slice(j * LANES, (j + 1) * LANES)
                total = chosen[:, lanes] + acc[plan.place(h, m, j)]
                out[m, :, lanes] = total.astype(out.dtype)


def local(trial, energy_gap, coulomb_factors, occ_values, vir_values, kernel, live_points, sizes):
    plan = Plan(sizes, trial, coulomb_factors, occ_values, vir_values)
    groups, blks, vecs, k = plan.groups, plan.blks, plan.vecs, plan.k
    batches, points, virs, occs = plan.batches, plan.points, plan.virs, plan.occs
    digits = digits_of(blks)
    half = (plan.count, k, plan.length)
    bf16, f32 = jnp.bfloat16, jnp.float32

    def bind(body, *first):
        return lambda *refs: body(plan, *first, *refs)

    trial_cols = trial.T
    start = call(
        bind(head_kernel), shape(trial_cols.shape, bf16), [VMEM], flops=HEAD, name="head"
    )(trial_cols)
    pieces, masks = [trial_cols], [0]
    for stride, radix in reversed(digits):
        known = len(masks)
        for d in range(1, radix):
            for n in range(known):
                pieces.append(swap(pieces[n], "blk", blks, d * stride))
                masks.append(masks[n] ^ (d * stride))
    pieces[0] = start
    pieces = [p for _, p in sorted(zip(masks, pieces), key=lambda pair: pair[0])]

    if plan.aligned:
        mine = call(bind(stack_kernel), shape(half, bf16), [VMEM] * len(pieces), name="stack")(
            *pieces
        )
        other = swap(mine, "vec", vecs, 1)
    else:
        me, vec = lax.axis_index("blk"), lax.axis_index("vec")
        mine = jnp.take(jnp.stack(pieces), me ^ jnp.arange(blks), axis=0)
        both = jnp.stack([mine, swap(mine, "vec", vecs, 1)])
        both = jnp.take(both, vec ^ jnp.arange(vecs), axis=0)
        both = both.transpose(2, 1, 0, 3).reshape(k, vecs, plan.length)
        mine, other = both[None, :, 0], both[None, :, 1]

    flops = 2 * k * plan.aux * plan.pairs
    grid_flops = 2 * batches * points * virs * occs * k
    occ_scratch = pltpu.VMEM((batches, plan.occ_all, points), f32)
    dens, sent = call(
        bind(dens_kernel),
        (
            shape((batches, k, points), f32),
            shape((batches, k, points), bf16),
        ),
        [VMEM] * 4,
        grid_flops,
        [
            pltpu.VMEM((occs * k, virs), bf16),
            occ_scratch,
        ],
        name="dens",
    )(mine, other, vir_values, occ_values)
    other_dens = swap(sent, "grp", groups, 1)

    part = call(
        bind(fac_kernel),
        shape((k, plan.aux), f32),
        [VMEM] * 3,
        flops,
        [pltpu.VMEM((k, plan.pairs), bf16)],
        name="fac",
    )(mine, other, coulomb_factors)
    other_part = swap(part, "grp", groups, 1)

    acc = call(
        bind(grid_kernel),
        shape((occs * k, virs), f32),
        [SMEM] + [VMEM] * 5,
        grid_flops,
        [pltpu.VMEM((occs * k, points), bf16), occ_scratch],
        name="grid",
    )(live_points, dens, other_dens, occ_values, kernel, vir_values)
    stay, sent = call(
        bind(back_kernel), (shape(half, f32), shape(half, bf16)), [VMEM] * 4, flops, name="back"
    )(part, other_part, coulomb_factors, acc)

    if plan.aligned:
        total = stay + swap(sent, "vec", vecs, 1).astype(f32)
    else:
        full = jnp.concatenate([stay[0], sent[0].astype(f32)], axis=1)
        full = full.reshape(k, blks, vecs, plan.rows).transpose(2, 1, 0, 3)
        full = jnp.take(full, me ^ jnp.arange(blks), axis=1)
        full = jnp.take(full, vec ^ jnp.arange(vecs), axis=0)
        total = full[0] + swap(full[1].astype(bf16), "vec", vecs, 1).astype(f32)

    for stride, radix in digits:
        total = total.reshape((-1, radix) + total.shape[1:])
        came = [
            swap(total[:, d].astype(bf16), "blk", blks, d * stride).astype(f32)
            for d in range(1, radix)
        ]
        total = sum(came, total[:, 0])
    result = energy_gap[None, :] * start.astype(f32) + total[0]
    return result.astype(bf16).T


def solution(mesh):
    sizes = tuple(mesh.shape[a] for a in ("grp", "blk", "vec"))
    in_specs = (
        P(("grp", "blk", "vec"), None),
        P(("grp", "blk", "vec")),
        P("blk", None),
        P("blk", None, None),
        P("blk", None, None),
        P("blk", None),
        P("blk"),
    )
    out_specs = P(("grp", "blk", "vec"), None)

    def program(*args):
        return local(*args, sizes=sizes)

    return jax.shard_map(program, mesh=mesh, in_specs=in_specs, out_specs=out_specs, check_vma=False)
```

```python
import jax
import jax.numpy as jnp
from jax import lax
from jax.experimental import pallas as pl
from jax.experimental.pallas import tpu as pltpu
from jax.sharding import PartitionSpec as P


LANES = 128
HEAD = 10**10
NT = (((1,), (1,)), ((), ()))
NN = (((1,), (0,)), ((), ()))
VMEM = pl.BlockSpec(memory_space=pltpu.VMEM)
SMEM = pl.BlockSpec(memory_space=pltpu.SMEM)
ANY = pl.BlockSpec(memory_space=pl.ANY)


def digits_of(count):
    digits, stride = [], 1
    bits = count.bit_length() - 1
    if bits % 2:
        digits.append((1, 2))
        stride = 2
    while stride < count:
        digits.append((stride, 4))
        stride *= 4
    return digits


def swap(x, axis, count, mask):
    return lax.ppermute(x, axis, [(i, i ^ mask) for i in range(count)])


def call(body, out_shape, in_specs, flops=0, scratch=(), limit=14):
    return pl.pallas_call(
        body,
        out_shape=out_shape,
        in_specs=in_specs,
        out_specs=jax.tree.map(lambda _: VMEM, out_shape),
        scratch_shapes=list(scratch),
        compiler_params=pltpu.CompilerParams(vmem_limit_bytes=limit * 2**20),
        cost_estimate=pl.CostEstimate(flops=flops, bytes_accessed=0, transcendentals=0),
    )


def after(body, count):
    return lambda *refs: body(*refs[:count], *refs[count + 1 :])


def shape(dims, dtype):
    return jax.ShapeDtypeStruct(dims, dtype)


class Plan:
    def __init__(self, sizes, trial, coulomb_factors, occ_values, vir_values):
        self.groups, self.blks, self.vecs = sizes
        self.rows, self.k = trial.shape
        self.aux = coulomb_factors.shape[0] // self.vecs
        self.pairs = coulomb_factors.shape[1] // self.groups
        self.batches = occ_values.shape[0] // self.vecs
        self.occ_all, self.points = occ_values.shape[1:]
        self.occs = self.occ_all // self.groups
        self.virs = vir_values.shape[2]
        self.aligned = self.rows % LANES == 0
        self.count = self.blks if self.aligned else 1
        self.length = self.rows if self.aligned else self.pairs // self.vecs
        self.per = self.length // LANES
        self.digits = digits_of(self.blks)
        stride, radix = self.digits[-1]
        self.top = stride
        if self.aligned and radix == 4 and len(self.digits) == 2 and self.occs % radix == 0:
            self.parts = [(2, 3), (0, 1)]
            self.run = self.occs // radix
        else:
            assert not self.aligned
            self.parts = [(0,)]
            self.run = self.occs

    def masks(self, part):
        if len(self.parts) == 1:
            return list(range(self.count))
        return [d * self.top + low for d in part for low in range(self.top)]

    def first_row(self, d):
        return (lax.axis_index("blk") // self.top ^ d) * self.run if len(self.parts) > 1 else 0

    def owner(self, m):
        return lax.axis_index("blk") ^ m if self.aligned else 0

    def part(self, h):
        return lax.axis_index("vec") ^ h if self.aligned else h

    def block(self, h, m, j):
        return (self.owner(m) * self.vecs + self.part(h)) * self.per + j

    def place(self, h, m, j):
        at = self.block(h, m, j)
        tiles = self.virs // LANES
        return (
            pl.ds(pl.multiple_of((at // tiles) * self.k, self.k), self.k),
            pl.ds(pl.multiple_of((at % tiles) * LANES, LANES), LANES),
        )


def copy_kernel(plan, given, out):
    out[...] = given[...]


def stack_kernel(plan, *refs):
    for m, piece in enumerate(refs[:-1]):
        refs[-1][m] = piece[...]


def occ_rows(plan, occ, b, occ32):
    occ32[...] = occ[lax.axis_index("vec") * plan.batches + b].astype(jnp.float32)
    base = lax.axis_index("grp") * plan.occs
    return lambda i: occ32[pl.ds(base + i, 1), :]


def factor_block(plan, fac, m, p):
    top = pl.multiple_of(lax.axis_index("vec") * plan.aux, plan.aux)
    at = lax.axis_index("grp") * plan.pairs + (plan.owner(m) * plan.vecs + p) * plan.length
    return fac[pl.ds(top, plan.aux), pl.ds(pl.multiple_of(at, LANES), plan.length)]


def rows_kernel(plan, mine, other, rows):
    for h, half in enumerate((mine, other)):
        for m in range(plan.count):
            for j in range(plan.per):
                rows[plan.place(h, m, j)] = half[m, :, j * LANES : (j + 1) * LANES]


def dens_kernel(plan, span, rows, vir, occ, dens, sent, occ32):
    k = plan.k
    vec = lax.axis_index("vec")
    for n, b in enumerate(span):
        row = occ_rows(plan, occ, b, occ32.at[n])
        trans = lax.dot_general(
            rows[...], vir[vec * plan.batches + b], NT, preferred_element_type=jnp.float32
        )
        total = row(0) * trans[:k, :]
        for i in range(1, plan.occs):
            total = total + row(i) * trans[i * k : (i + 1) * k, :]
        dens[n] = total
        sent[n] = total.astype(sent.dtype)


def first_dens_kernel(plan, span, mine, other, vir, occ, dens, sent, rows, occ32):
    rows_kernel(plan, mine, other, rows)
    dens_kernel(plan, span, rows, vir, occ, dens, sent, occ32)


def fac_kernel(plan, h, half, fac, *refs):
    value = refs[0][...] if len(refs) > 1 else 0.0
    for m in range(plan.count):
        value += lax.dot_general(
            half[m], factor_block(plan, fac, m, plan.part(h)), NT, preferred_element_type=jnp.float32
        )
    refs[-1][...] = value


def grid_kernel(plan, part, spans, live, *refs):
    count = len(spans)
    pairs = refs[: 2 * count]
    occ, weight, vir, acc, scaled, occ32 = refs[2 * count :]
    k = plan.k
    base = lax.axis_index("vec") * plan.batches
    slots = lax.broadcasted_iota(jnp.int32, (1, plan.points), 1)
    for c, span in enumerate(spans):
        for n, b in enumerate(span):
            row = occ_rows(plan, occ, b, occ32.at[b])
            density = pairs[2 * c][n] + pairs[2 * c + 1][n].astype(jnp.float32)
            used = jnp.where(slots < live[base + b], weight[pl.ds(base + b, 1), :], 0.0)
            weighted = density * used
            for t, d in enumerate(part):
                first = plan.first_row(d)
                for r in range(plan.run):
                    at = (t * plan.run + r) * k
                    scaled[at : at + k, :] = (row(first + r) * weighted).astype(jnp.bfloat16)
            value = lax.dot_general(
                scaled[...], vir[base + b], NN, preferred_element_type=jnp.float32
            )
            if b == 0:
                acc[...] = value
            else:
                acc[...] += value


def back_kernel(plan, part, part_a, part_b, fac, acc, stay, sent):
    both = (part_a[...] + part_b[...]).astype(jnp.bfloat16)
    k, tiles = plan.k, plan.virs // LANES
    masks = plan.masks(part)
    for n, m in enumerate(masks):
        t = n * len(part) // len(masks)
        first = plan.first_row(part[t])
        for h, out in enumerate((stay, sent)):
            value = 2.0 * lax.dot_general(
                both,
                factor_block(plan, fac, m, plan.part(h)),
                NN,
                preferred_element_type=jnp.float32,
            )
            for j in range(plan.per):
                at = plan.block(h, m, j)
                row = (at // tiles - first + t * plan.run) * k
                found = acc[
                    pl.ds(pl.multiple_of(row, k), k),
                    pl.ds(pl.multiple_of((at % tiles) * LANES, LANES), LANES),
                ]
                lanes = slice(j * LANES, (j + 1) * LANES)
                out[n, :, lanes] = (value[:, lanes] + found).astype(out.dtype)


def sum_kernel(plan, radix, stay, came, *outs):
    for n in range(stay.shape[0]):
        out = outs[n % radix]
        out[n // radix] = (stay[n] + came[n].astype(jnp.float32)).astype(out.dtype)


def split_kernel(plan, own, *refs):
    outs = refs[-own.shape[0] :]
    for n, out in enumerate(outs):
        total = own[n]
        for came in refs[: -len(outs)]:
            total = total + came[n].astype(jnp.float32)
        out[...] = total.astype(out.dtype)


def local(trial, energy_gap, coulomb_factors, occ_values, vir_values, kernel, live_points, sizes):
    plan = Plan(sizes, trial, coulomb_factors, occ_values, vir_values)
    groups, blks, vecs, k = plan.groups, plan.blks, plan.vecs, plan.k
    batches, points, virs, occs = plan.batches, plan.points, plan.virs, plan.occs
    digits = plan.digits
    half = (plan.count, k, plan.length)
    bf16, f32 = jnp.bfloat16, jnp.float32

    def bind(body, *first):
        return lambda *refs: body(plan, *first, *refs)

    trial_cols = trial.T
    pieces, masks = [trial_cols], [0]
    for stride, radix in reversed(digits):
        known = len(masks)
        for d in range(1, radix):
            for n in range(known):
                pieces.append(swap(pieces[n], "blk", blks, d * stride))
                masks.append(masks[n] ^ (d * stride))
        if known == 1:
            pieces[-1] = call(
                bind(copy_kernel), shape(trial_cols.shape, bf16), [VMEM], flops=HEAD
            )(pieces[-1])
    pieces = [p for _, p in sorted(zip(masks, pieces), key=lambda pair: pair[0])]

    if plan.aligned:
        mine = call(bind(stack_kernel), shape(half, bf16), [VMEM] * len(pieces))(*pieces)
        other = swap(mine, "vec", vecs, 1)
    else:
        me, vec = lax.axis_index("blk"), lax.axis_index("vec")
        mine = jnp.take(jnp.stack(pieces), me ^ jnp.arange(blks), axis=0)
        both = jnp.stack([mine, swap(mine, "vec", vecs, 1)])
        both = jnp.take(both, vec ^ jnp.arange(vecs), axis=0)
        both = both.transpose(2, 1, 0, 3).reshape(k, vecs, plan.length)
        mine, other = both[None, :, 0], both[None, :, 1]

    flops = k * plan.aux * plan.pairs
    part = call(bind(fac_kernel, 0), shape((k, plan.aux), f32), [VMEM] * 2, flops)(
        mine, coulomb_factors
    )

    cut = (batches + 1) // 2
    spans = [tuple(range(cut)), tuple(range(cut, batches))]
    grid_flops = 2 * points * virs * occs * k
    occ_scratch = pltpu.VMEM((batches, plan.occ_all, points), f32)
    rows = None
    density = []
    for span in spans:
        chunk = (len(span), k, points)
        out = (shape(chunk, f32), shape(chunk, bf16))
        if rows is None:
            dens, sent, rows = call(
                after(bind(first_dens_kernel, span), 4),
                out + (shape((occs * k, virs), bf16),),
                [VMEM] * 4 + [ANY],
                grid_flops * len(span),
                [occ_scratch],
            )(mine, other, vir_values, occ_values, part)
        else:
            dens, sent = call(
                bind(dens_kernel, span), out, [VMEM] * 3, grid_flops * len(span), [occ_scratch]
            )(rows, vir_values, occ_values)
        density += [dens, swap(sent, "grp", groups, 1)]

    part = call(bind(fac_kernel, 1), shape((k, plan.aux), f32), [VMEM] * 3, flops)(
        other, coulomb_factors, part
    )
    other_part = swap(part, "grp", groups, 1)

    def grid(number, *order):
        chosen = plan.parts[number]
        used = plan.run * len(chosen)
        body = bind(grid_kernel, chosen, spans)
        return call(
            after(body, len(density) + 4) if order else body,
            shape((used * k, virs), f32),
            [SMEM] + [VMEM] * (len(density) + 3) + [ANY] * len(order),
            grid_flops * batches * used // occs,
            [pltpu.VMEM((used * k, points), bf16), occ_scratch],
        )(live_points, *density, occ_values, kernel, vir_values, *order)

    def back(number, acc, *order):
        chosen = plan.parts[number]
        share = (len(plan.masks(chosen)),) + half[1:]
        body = bind(back_kernel, chosen)
        return call(
            after(body, 4) if order else body,
            (shape(share, f32), shape(share, bf16)),
            [VMEM] * 4 + [ANY] * len(order),
            2 * flops // len(plan.parts),
        )(part, other_part, coulomb_factors, acc, *order)

    if len(plan.parts) == 2:
        (stride, radix), (top, _) = digits
        count = plan.count // 2

        def first_sum(stay, sent, *order):
            body = bind(sum_kernel, radix)
            return call(
                after(body, 2) if order else body,
                (shape((count // radix,) + half[1:], f32),)
                + (shape((count // radix,) + half[1:], bf16),) * (radix - 1),
                [VMEM] * 2 + [ANY] * len(order),
            )(stay, swap(sent, "vec", vecs, 1), *order)

        def next_sum(number, own, sends):
            came = [swap(x, "blk", blks, (d + 1) * stride) for d, x in enumerate(sends)]
            out = [shape(half[1:], bf16 if d else f32) for d in plan.parts[number]]
            outs = call(bind(split_kernel), out, [VMEM] * (1 + len(came)))(own, *came)
            return [
                swap(x, "blk", blks, d * top) if d else x
                for d, x in zip(plan.parts[number], outs)
            ]

        acc = grid(0)
        stay, sent = back(0, acc)
        acc = grid(1, stay)
        far = first_sum(stay, sent, acc)
        stay, sent = back(1, acc, far[0])
        near = first_sum(stay, sent)
        came = next_sum(0, far[0], far[1:]) + next_sum(1, near[0], near[1:])
    else:
        stay, sent = back(0, grid(0))
        full = jnp.concatenate([stay[0], sent[0].astype(f32)], axis=1)
        full = full.reshape(k, blks, vecs, plan.rows).transpose(2, 1, 0, 3)
        full = jnp.take(full, me ^ jnp.arange(blks), axis=1)
        full = jnp.take(full, vec ^ jnp.arange(vecs), axis=0)
        total = full[0] + swap(full[1].astype(bf16), "vec", vecs, 1).astype(f32)
        for stride, radix in digits:
            total = total.reshape((-1, radix) + total.shape[1:])
            total = sum(
                (
                    swap(total[:, d].astype(bf16), "blk", blks, d * stride).astype(f32)
                    for d in range(1, radix)
                ),
                total[:, 0],
            )
        came = [total[0]]
    total = sum((x.astype(f32) for x in came[1:]), came[0].astype(f32))
    result = energy_gap[None, :] * trial_cols.astype(f32) + total
    return result.astype(bf16).T


def solution(mesh):
    sizes = tuple(mesh.shape[a] for a in ("grp", "blk", "vec"))
    in_specs = (
        P(("grp", "blk", "vec"), None),
        P(("grp", "blk", "vec")),
        P("blk", None),
        P("blk", None, None),
        P("blk", None, None),
        P("blk", None),
        P("blk"),
    )
    out_specs = P(("grp", "blk", "vec"), None)

    def program(*args):
        return local(*args, sizes=sizes)

    return jax.shard_map(
        program, mesh=mesh, in_specs=in_specs, out_specs=out_specs, check_vma=False
    )
```

```python
import jax
import jax.numpy as jnp
from jax import lax
from jax.experimental import pallas as pl
from jax.experimental.pallas import tpu as pltpu
from jax.sharding import PartitionSpec as P


LANES = 128
HEAD = 10**10
NT = (((1,), (1,)), ((), ()))
NN = (((1,), (0,)), ((), ()))
VMEM = pl.BlockSpec(memory_space=pltpu.VMEM)
SMEM = pl.BlockSpec(memory_space=pltpu.SMEM)
ANY = pl.BlockSpec(memory_space=pl.ANY)


def digits_of(count):
    digits, stride = [], 1
    bits = count.bit_length() - 1
    if bits % 2:
        digits.append((1, 2))
        stride = 2
    while stride < count:
        digits.append((stride, 4))
        stride *= 4
    return digits


def swap(x, axis, count, mask):
    return lax.ppermute(x, axis, [(i, i ^ mask) for i in range(count)])


def call(body, out_shape, in_specs, flops=0, scratch=(), limit=14):
    return pl.pallas_call(
        body,
        out_shape=out_shape,
        in_specs=in_specs,
        out_specs=jax.tree.map(lambda _: VMEM, out_shape),
        scratch_shapes=list(scratch),
        compiler_params=pltpu.CompilerParams(vmem_limit_bytes=limit * 2**20),
        cost_estimate=pl.CostEstimate(flops=flops, bytes_accessed=0, transcendentals=0),
    )


def after(body, count):
    return lambda *refs: body(*refs[:count], *refs[count + 1 :])


def shape(dims, dtype):
    return jax.ShapeDtypeStruct(dims, dtype)


class Plan:
    def __init__(self, sizes, trial, coulomb_factors, occ_values, vir_values):
        self.groups, self.blks, self.vecs = sizes
        self.rows, self.k = trial.shape
        self.aux = coulomb_factors.shape[0] // self.vecs
        self.pairs = coulomb_factors.shape[1] // self.groups
        self.batches = occ_values.shape[0] // self.vecs
        self.occ_all, self.points = occ_values.shape[1:]
        self.occs = self.occ_all // self.groups
        self.virs = vir_values.shape[2]
        self.aligned = self.rows % LANES == 0
        self.count = self.blks if self.aligned else 1
        self.length = self.rows if self.aligned else self.pairs // self.vecs
        self.per = self.length // LANES
        self.digits = digits_of(self.blks)
        stride, radix = self.digits[-1]
        self.top = stride
        if self.aligned and radix == 4 and len(self.digits) == 2 and self.occs % radix == 0:
            self.parts = [(2, 3), (0, 1)]
            self.run = self.occs // radix
        else:
            assert not self.aligned
            self.parts = [(0,)]
            self.run = self.occs

        if 2 * self.aux <= self.points and self.aux % LANES == 0:
            self.packed = [(0, 0), (0, self.aux)]
        else:
            self.packed = [(0, 0), (1, 0)]
        self.slots = self.packed[-1][0] + 1

    def masks(self, part):
        if len(self.parts) == 1:
            return list(range(self.count))
        return [d * self.top + low for d in part for low in range(self.top)]

    def first_row(self, d):
        return (lax.axis_index("blk") // self.top ^ d) * self.run if len(self.parts) > 1 else 0

    def owner(self, m):
        return lax.axis_index("blk") ^ m if self.aligned else 0

    def part(self, h):
        return lax.axis_index("vec") ^ h if self.aligned else h

    def block(self, h, m, j):
        return (self.owner(m) * self.vecs + self.part(h)) * self.per + j

    def place(self, h, m, j):
        at = self.block(h, m, j)
        tiles = self.virs // LANES
        return (
            pl.ds(pl.multiple_of((at // tiles) * self.k, self.k), self.k),
            pl.ds(pl.multiple_of((at % tiles) * LANES, LANES), LANES),
        )


def copy_kernel(plan, given, out):
    out[...] = given[...]


def stack_kernel(plan, *refs):
    for m, piece in enumerate(refs[:-1]):
        refs[-1][m] = piece[...]


def occ_rows(plan, occ, b, occ32):
    occ32[...] = occ[lax.axis_index("vec") * plan.batches + b].astype(jnp.float32)
    base = lax.axis_index("grp") * plan.occs
    return lambda i: occ32[pl.ds(base + i, 1), :]


def factor_block(plan, fac, m, p):
    top = pl.multiple_of(lax.axis_index("vec") * plan.aux, plan.aux)
    at = lax.axis_index("grp") * plan.pairs + (plan.owner(m) * plan.vecs + p) * plan.length
    return fac[pl.ds(top, plan.aux), pl.ds(pl.multiple_of(at, LANES), plan.length)]


def rows_kernel(plan, mine, other, rows):
    for h, half in enumerate((mine, other)):
        for m in range(plan.count):
            for j in range(plan.per):
                rows[plan.place(h, m, j)] = half[m, :, j * LANES : (j + 1) * LANES]


def dens_kernel(plan, span, rows, vir, occ, dens, sent, occ32):
    k = plan.k
    vec = lax.axis_index("vec")
    for n, b in enumerate(span):
        row = occ_rows(plan, occ, b, occ32.at[n])
        trans = lax.dot_general(
            rows[...], vir[vec * plan.batches + b], NT, preferred_element_type=jnp.float32
        )
        total = row(0) * trans[:k, :]
        for i in range(1, plan.occs):
            total = total + row(i) * trans[i * k : (i + 1) * k, :]
        dens[n] = total
        sent[n] = total.astype(sent.dtype)


def first_dens_kernel(plan, span, mine, other, vir, occ, dens, sent, rows, occ32):
    rows_kernel(plan, mine, other, rows)
    dens_kernel(plan, span, rows, vir, occ, dens, sent, occ32)


def fac_kernel(plan, h, half, fac, *refs):
    value = refs[0][...] if len(refs) > 1 else 0.0
    for m in range(plan.count):
        value += lax.dot_general(
            half[m], factor_block(plan, fac, m, plan.part(h)), NT, preferred_element_type=jnp.float32
        )
    refs[-1][...] = value


def second_dens_kernel(plan, span, rows, vir, occ, other, fac, part, dens, sent, total, occ32):
    dens_kernel(plan, span, rows, vir, occ, dens, sent, occ32)
    fac_kernel(plan, 1, other, fac, part, total)
    value = total[...]
    if 2 * plan.aux < plan.slots * plan.points:
        for slot in range(plan.slots):
            sent[len(span) + slot] = jnp.zeros(sent.shape[1:], sent.dtype)
    for slot, lane in plan.packed:
        term = value.astype(sent.dtype)
        sent[len(span) + slot, :, lane : lane + plan.aux] = term
        value = value - term.astype(jnp.float32)


def grid_kernel(plan, part, span, skip, live, dens_a, dens_b, occ, weight, vir, *refs):
    acc, scaled, occ32 = refs[-3:]
    k = plan.k
    base = lax.axis_index("vec") * plan.batches
    slots = lax.broadcasted_iota(jnp.int32, (1, plan.points), 1)
    for n, b in enumerate(span):
        row = occ_rows(plan, occ, b, occ32.at[n])
        density = dens_a[n] + dens_b[n].astype(jnp.float32)
        used = jnp.where(slots < live[base + b], weight[pl.ds(base + b, 1), :], 0.0)
        weighted = density * used
        for t, d in enumerate(part):
            first = plan.first_row(d)
            for r in range(plan.run):
                at = (t * plan.run + r) * k
                scaled[at : at + k, :] = (row(first + r) * weighted).astype(jnp.bfloat16)
        value = lax.dot_general(scaled[...], vir[base + b], NN, preferred_element_type=jnp.float32)
        if n:
            acc[...] += value
        elif skip is None:
            acc[...] = value
        else:
            acc[...] = refs[0][pl.ds(skip, acc.shape[0]), :] + value


def back_kernel(plan, part, part_a, part_b, fac, acc, stay, sent):
    both = part_a[...]
    first = part_b.shape[0] - plan.slots
    for slot, lane in plan.packed:
        both = both + part_b[first + slot, :, lane : lane + plan.aux].astype(jnp.float32)
    both = both.astype(jnp.bfloat16)
    k, tiles = plan.k, plan.virs // LANES
    masks = plan.masks(part)
    for n, m in enumerate(masks):
        t = n * len(part) // len(masks)
        first = plan.first_row(part[t])
        for h, out in enumerate((stay, sent)):
            value = 2.0 * lax.dot_general(
                both,
                factor_block(plan, fac, m, plan.part(h)),
                NN,
                preferred_element_type=jnp.float32,
            )
            for j in range(plan.per):
                at = plan.block(h, m, j)
                row = (at // tiles - first + t * plan.run) * k
                found = acc[
                    pl.ds(pl.multiple_of(row, k), k),
                    pl.ds(pl.multiple_of((at % tiles) * LANES, LANES), LANES),
                ]
                lanes = slice(j * LANES, (j + 1) * LANES)
                out[n, :, lanes] = (value[:, lanes] + found).astype(out.dtype)


def sum_kernel(plan, radix, stay, came, *outs):
    for n in range(stay.shape[0]):
        out = outs[n % radix]
        out[n // radix] = (stay[n] + came[n].astype(jnp.float32)).astype(out.dtype)


def split_kernel(plan, own, *refs):
    outs = refs[-own.shape[0] :]
    for n, out in enumerate(outs):
        total = own[n]
        for came in refs[: -len(outs)]:
            total = total + came[n].astype(jnp.float32)
        out[...] = total.astype(out.dtype)


def local(trial, energy_gap, coulomb_factors, occ_values, vir_values, kernel, live_points, sizes):
    plan = Plan(sizes, trial, coulomb_factors, occ_values, vir_values)
    groups, blks, vecs, k = plan.groups, plan.blks, plan.vecs, plan.k
    batches, points, virs, occs = plan.batches, plan.points, plan.virs, plan.occs
    digits = plan.digits
    half = (plan.count, k, plan.length)
    bf16, f32 = jnp.bfloat16, jnp.float32

    def bind(body, *first):
        return lambda *refs: body(plan, *first, *refs)

    trial_cols = trial.T
    pieces, masks = [trial_cols], [0]
    for stride, radix in reversed(digits):
        known = len(masks)
        for d in range(1, radix):
            for n in range(known):
                pieces.append(swap(pieces[n], "blk", blks, d * stride))
                masks.append(masks[n] ^ (d * stride))
        if known == 1:
            pieces[-1] = call(
                bind(copy_kernel), shape(trial_cols.shape, bf16), [VMEM], flops=HEAD
            )(pieces[-1])
    pieces = [p for _, p in sorted(zip(masks, pieces), key=lambda pair: pair[0])]

    if plan.aligned:
        mine = call(
            after(bind(stack_kernel), 0), shape(half, bf16), [VMEM] * (len(pieces) + 1)
        )(vir_values, *pieces)
        other = swap(mine, "vec", vecs, 1)
    else:
        me, vec = lax.axis_index("blk"), lax.axis_index("vec")
        mine = jnp.take(jnp.stack(pieces), me ^ jnp.arange(blks), axis=0)
        both = jnp.stack([mine, swap(mine, "vec", vecs, 1)])
        both = jnp.take(both, vec ^ jnp.arange(vecs), axis=0)
        both = both.transpose(2, 1, 0, 3).reshape(k, vecs, plan.length)
        mine, other = both[None, :, 0], both[None, :, 1]

    flops = k * plan.aux * plan.pairs
    part = call(bind(fac_kernel, 0), shape((k, plan.aux), f32), [VMEM] * 2, flops)(
        mine, coulomb_factors
    )

    cut = (batches + 1) // 2
    spans = [tuple(range(cut)), tuple(range(cut, batches))]
    chunks = [(len(span), k, points) for span in spans]
    grid_flops = 2 * points * virs * occs * k

    def occ_scratch(span):
        return pltpu.VMEM((len(span), plan.occ_all, points), f32)

    first_dens, sent, rows = call(
        after(bind(first_dens_kernel, spans[0]), 4),
        (shape(chunks[0], f32), shape(chunks[0], bf16), shape((occs * k, virs), bf16)),
        [VMEM] * 4 + [ANY],
        grid_flops * len(spans[0]),
        [occ_scratch(spans[0])],
    )(mine, other, vir_values, occ_values, part)
    first_other = swap(sent, "grp", groups, 1)
    second_dens, sent, part = call(
        bind(second_dens_kernel, spans[1]),
        (
            shape(chunks[1], f32),
            shape((len(spans[1]) + plan.slots, k, points), bf16),
            shape((k, plan.aux), f32),
        ),
        [VMEM] * 6,
        grid_flops * len(spans[1]) + flops,
        [occ_scratch(spans[1])],
    )(rows, vir_values, occ_values, other, coulomb_factors, part)
    second_other = swap(sent, "grp", groups, 1)

    def grid(chosen, chunk, dens, came, skip, *more):
        used = plan.run * len(chosen)
        count = 6 + (skip is not None)
        body = bind(grid_kernel, chosen, spans[chunk], skip)
        return call(
            after(body, count) if len(more) + 6 > count else body,
            shape((used * k, virs), f32),
            [SMEM] + [VMEM] * (count - 1) + [ANY] * (len(more) + 6 - count),
            grid_flops * len(spans[chunk]) * used // occs,
            [pltpu.VMEM((used * k, points), bf16), occ_scratch(spans[chunk])],
        )(live_points, dens, came, occ_values, kernel, vir_values, *more)

    every = sum(plan.parts, ())
    begun = grid(every, 0, first_dens, first_other, None, sent)

    def finish(number, *order):
        skip = sum(len(chosen) for chosen in plan.parts[:number]) * plan.run * k
        return grid(plan.parts[number], 1, second_dens, second_other, skip, begun, *order)

    def back(number, acc, *order):
        chosen = plan.parts[number]
        share = (len(plan.masks(chosen)),) + half[1:]
        body = bind(back_kernel, chosen)
        return call(
            after(body, 4) if order else body,
            (shape(share, f32), shape(share, bf16)),
            [VMEM] * 4 + [ANY] * len(order),
            2 * flops // len(plan.parts),
        )(part, second_other, coulomb_factors, acc, *order)

    if len(plan.parts) == 2:
        (stride, radix), (top, _) = digits
        count = plan.count // 2

        def first_sum(stay, sent, *order):
            body = bind(sum_kernel, radix)
            return call(
                after(body, 2) if order else body,
                (shape((count // radix,) + half[1:], f32),)
                + (shape((count // radix,) + half[1:], bf16),) * (radix - 1),
                [VMEM] * 2 + [ANY] * len(order),
            )(stay, swap(sent, "vec", vecs, 1), *order)

        def next_sum(number, own, sends):
            came = [swap(x, "blk", blks, (d + 1) * stride) for d, x in enumerate(sends)]
            out = [shape(half[1:], bf16 if d else f32) for d in plan.parts[number]]
            outs = call(bind(split_kernel), out, [VMEM] * (1 + len(came)))(own, *came)
            return [
                swap(x, "blk", blks, d * top) if d else x
                for d, x in zip(plan.parts[number], outs)
            ]

        stay, sent = back(0, finish(0))
        acc = finish(1, stay)
        far = first_sum(stay, sent, acc)
        stay, sent = back(1, acc, far[0])
        near = first_sum(stay, sent)
        came = next_sum(0, far[0], far[1:]) + next_sum(1, near[0], near[1:])
    else:
        stay, sent = back(0, finish(0))
        full = jnp.concatenate([stay[0], sent[0].astype(f32)], axis=1)
        full = full.reshape(k, blks, vecs, plan.rows).transpose(2, 1, 0, 3)
        full = jnp.take(full, me ^ jnp.arange(blks), axis=1)
        full = jnp.take(full, vec ^ jnp.arange(vecs), axis=0)
        total = full[0] + swap(full[1].astype(bf16), "vec", vecs, 1).astype(f32)
        for stride, radix in digits:
            total = total.reshape((-1, radix) + total.shape[1:])
            total = sum(
                (
                    swap(total[:, d].astype(bf16), "blk", blks, d * stride).astype(f32)
                    for d in range(1, radix)
                ),
                total[:, 0],
            )
        came = [total[0]]
    total = sum((x.astype(f32) for x in came[1:]), came[0].astype(f32))
    result = energy_gap[None, :] * trial_cols.astype(f32) + total
    return result.astype(bf16).T


def solution(mesh):
    sizes = tuple(mesh.shape[a] for a in ("grp", "blk", "vec"))
    in_specs = (
        P(("grp", "blk", "vec"), None),
        P(("grp", "blk", "vec")),
        P("blk", None),
        P("blk", None, None),
        P("blk", None, None),
        P("blk", None),
        P("blk"),
    )
    out_specs = P(("grp", "blk", "vec"), None)

    def program(*args):
        return local(*args, sizes=sizes)

    return jax.shard_map(
        program, mesh=mesh, in_specs=in_specs, out_specs=out_specs, check_vma=False
    )
```

```python
import jax
import jax.numpy as jnp
from jax import lax
from jax.experimental import pallas as pl
from jax.experimental.pallas import tpu as pltpu
from jax.sharding import PartitionSpec as P


LANES = 128
HEAD = 10**10
NT = (((1,), (1,)), ((), ()))
NN = (((1,), (0,)), ((), ()))
VMEM = pl.BlockSpec(memory_space=pltpu.VMEM)
SMEM = pl.BlockSpec(memory_space=pltpu.SMEM)
ANY = pl.BlockSpec(memory_space=pl.ANY)


def digits_of(count):
    digits, stride = [], 1
    bits = count.bit_length() - 1
    if bits % 2:
        digits.append((1, 2))
        stride = 2
    while stride < count:
        digits.append((stride, 4))
        stride *= 4
    return digits


def swap(x, axis, count, mask):
    return lax.ppermute(x, axis, [(i, i ^ mask) for i in range(count)])


def call(body, out_shape, in_specs, flops=0, scratch=(), limit=14):
    return pl.pallas_call(
        body,
        out_shape=out_shape,
        in_specs=in_specs,
        out_specs=jax.tree.map(lambda _: VMEM, out_shape),
        scratch_shapes=list(scratch),
        compiler_params=pltpu.CompilerParams(vmem_limit_bytes=limit * 2**20),
        cost_estimate=pl.CostEstimate(flops=flops, bytes_accessed=0, transcendentals=0),
    )


def after(body, count):
    return lambda *refs: body(*refs[:count], *refs[count + 1 :])


def shape(dims, dtype):
    return jax.ShapeDtypeStruct(dims, dtype)


class Plan:
    def __init__(self, sizes, trial, coulomb_factors, occ_values, vir_values):
        self.groups, self.blks, self.vecs = sizes
        self.rows, self.k = trial.shape
        self.aux = coulomb_factors.shape[0] // self.vecs
        self.pairs = coulomb_factors.shape[1] // self.groups
        self.batches = occ_values.shape[0] // self.vecs
        self.occ_all, self.points = occ_values.shape[1:]
        self.occs = self.occ_all // self.groups
        self.virs = vir_values.shape[2]
        self.aligned = self.rows % LANES == 0
        self.count = self.blks if self.aligned else 1
        self.length = self.rows if self.aligned else self.pairs // self.vecs
        self.per = self.length // LANES
        self.digits = digits_of(self.blks)
        stride, radix = self.digits[-1]
        self.top = stride
        if self.aligned and radix == 4 and len(self.digits) == 2 and self.occs % radix == 0:
            self.parts = [(3, 2), (0, 1)]
            self.run = self.occs // radix
        else:
            assert not self.aligned
            self.parts = [(0,)]
            self.run = self.occs

        if 2 * self.aux <= self.points and self.aux % LANES == 0:
            self.packed = [(0, 0), (0, self.aux)]
        else:
            self.packed = [(0, 0), (1, 0)]
        self.slots = self.packed[-1][0] + 1

    def masks(self, part):
        if len(self.parts) == 1:
            return list(range(self.count))
        return [d * self.top + low for d in part for low in range(self.top)]

    def first_row(self, d):
        return (lax.axis_index("blk") // self.top ^ d) * self.run if len(self.parts) > 1 else 0

    def owner(self, m):
        return lax.axis_index("blk") ^ m if self.aligned else 0

    def part(self, h):
        return lax.axis_index("vec") ^ h if self.aligned else h

    def block(self, h, m, j):
        return (self.owner(m) * self.vecs + self.part(h)) * self.per + j

    def place(self, h, m, j):
        at = self.block(h, m, j)
        tiles = self.virs // LANES
        return (
            pl.ds(pl.multiple_of((at // tiles) * self.k, self.k), self.k),
            pl.ds(pl.multiple_of((at % tiles) * LANES, LANES), LANES),
        )


def copy_kernel(plan, given, out):
    out[...] = given[...]


def stack_kernel(plan, *refs):
    for m, piece in enumerate(refs[:-1]):
        refs[-1][m] = piece[...]


def place_kernel(plan, slots, *refs):
    for slot, piece in zip(slots, refs):
        if isinstance(slot, tuple):
            for n, m in enumerate(slot):
                refs[-1][m] = piece[n]
        else:
            refs[-1][slot] = piece[...]


def occ_rows(plan, occ, b, occ32):
    occ32[...] = occ[lax.axis_index("vec") * plan.batches + b].astype(jnp.float32)
    base = lax.axis_index("grp") * plan.occs
    return lambda i: occ32[pl.ds(base + i, 1), :]


def factor_block(plan, fac, m, p):
    top = pl.multiple_of(lax.axis_index("vec") * plan.aux, plan.aux)
    at = lax.axis_index("grp") * plan.pairs + (plan.owner(m) * plan.vecs + p) * plan.length
    return fac[pl.ds(top, plan.aux), pl.ds(pl.multiple_of(at, LANES), plan.length)]


def rows_kernel(plan, mine, other, rows):
    for h, half in enumerate((mine, other)):
        for m in range(plan.count):
            for j in range(plan.per):
                rows[plan.place(h, m, j)] = half[m, :, j * LANES : (j + 1) * LANES]


def dens_kernel(plan, span, rows, vir, occ, dens, sent, occ32):
    k = plan.k
    vec = lax.axis_index("vec")
    for n, b in enumerate(span):
        row = occ_rows(plan, occ, b, occ32.at[n])
        trans = lax.dot_general(
            rows[...], vir[vec * plan.batches + b], NT, preferred_element_type=jnp.float32
        )
        total = row(0) * trans[:k, :]
        for i in range(1, plan.occs):
            total = total + row(i) * trans[i * k : (i + 1) * k, :]
        dens[n] = total
        sent[n] = total.astype(sent.dtype)


def first_dens_kernel(plan, span, mine, other, vir, occ, dens, sent, rows, occ32):
    rows_kernel(plan, mine, other, rows)
    dens_kernel(plan, span, rows, vir, occ, dens, sent, occ32)


def fac_kernel(plan, h, half, fac, *refs):
    value = refs[0][...] if len(refs) > 1 else 0.0
    for m in range(plan.count):
        value += lax.dot_general(
            half[m], factor_block(plan, fac, m, plan.part(h)), NT, preferred_element_type=jnp.float32
        )
    refs[-1][...] = value


def second_dens_kernel(plan, span, rows, vir, occ, other, fac, part, dens, sent, total, occ32):
    dens_kernel(plan, span, rows, vir, occ, dens, sent, occ32)
    fac_kernel(plan, 1, other, fac, part, total)
    value = total[...]
    if 2 * plan.aux < plan.slots * plan.points:
        for slot in range(plan.slots):
            sent[len(span) + slot] = jnp.zeros(sent.shape[1:], sent.dtype)
    for slot, lane in plan.packed:
        term = value.astype(sent.dtype)
        sent[len(span) + slot, :, lane : lane + plan.aux] = term
        value = value - term.astype(jnp.float32)


def grid_kernel(plan, part, span, skip, live, dens_a, dens_b, occ, weight, vir, *refs):
    acc, scaled, occ32 = refs[-3:]
    k = plan.k
    base = lax.axis_index("vec") * plan.batches
    slots = lax.broadcasted_iota(jnp.int32, (1, plan.points), 1)
    for n, b in enumerate(span):
        row = occ_rows(plan, occ, b, occ32.at[n])
        density = dens_a[n] + dens_b[n].astype(jnp.float32)
        used = jnp.where(slots < live[base + b], weight[pl.ds(base + b, 1), :], 0.0)
        weighted = density * used
        for t, d in enumerate(part):
            first = plan.first_row(d)
            for r in range(plan.run):
                at = (t * plan.run + r) * k
                scaled[at : at + k, :] = (row(first + r) * weighted).astype(jnp.bfloat16)
        value = lax.dot_general(scaled[...], vir[base + b], NN, preferred_element_type=jnp.float32)
        if n:
            acc[...] += value
        elif skip is None:
            acc[...] = value
        else:
            acc[...] = refs[0][pl.ds(skip, acc.shape[0]), :] + value


def back_kernel(plan, part, part_a, part_b, fac, acc, stay, sent):
    both = part_a[...]
    first = part_b.shape[0] - plan.slots
    for slot, lane in plan.packed:
        both = both + part_b[first + slot, :, lane : lane + plan.aux].astype(jnp.float32)
    both = both.astype(jnp.bfloat16)
    k, tiles = plan.k, plan.virs // LANES
    masks = plan.masks(part)
    for n, m in enumerate(masks):
        t = n * len(part) // len(masks)
        first = plan.first_row(part[t])
        for h, out in enumerate((stay, sent)):
            value = 2.0 * lax.dot_general(
                both,
                factor_block(plan, fac, m, plan.part(h)),
                NN,
                preferred_element_type=jnp.float32,
            )
            for j in range(plan.per):
                at = plan.block(h, m, j)
                row = (at // tiles - first + t * plan.run) * k
                found = acc[
                    pl.ds(pl.multiple_of(row, k), k),
                    pl.ds(pl.multiple_of((at % tiles) * LANES, LANES), LANES),
                ]
                lanes = slice(j * LANES, (j + 1) * LANES)
                out[n, :, lanes] = (value[:, lanes] + found).astype(out.dtype)


def sum_kernel(plan, radix, stay, came, *outs):
    for n in range(stay.shape[0]):
        out = outs[n % radix]
        out[n // radix] = (stay[n] + came[n].astype(jnp.float32)).astype(out.dtype)


def split_kernel(plan, own, *refs):
    outs = refs[-own.shape[0] :]
    for n, out in enumerate(outs):
        total = own[n]
        for came in refs[: -len(outs)]:
            total = total + came[n].astype(jnp.float32)
        out[...] = total.astype(out.dtype)


def local(trial, energy_gap, coulomb_factors, occ_values, vir_values, kernel, live_points, sizes):
    plan = Plan(sizes, trial, coulomb_factors, occ_values, vir_values)
    groups, blks, vecs, k = plan.groups, plan.blks, plan.vecs, plan.k
    batches, points, virs, occs = plan.batches, plan.points, plan.virs, plan.occs
    digits = plan.digits
    half = (plan.count, k, plan.length)
    bf16, f32 = jnp.bfloat16, jnp.float32

    def bind(body, *first):
        return lambda *refs: body(plan, *first, *refs)

    trial_cols = trial.T
    pieces, masks = [trial_cols], [0]
    for stride, radix in reversed(digits):
        known = len(masks)
        if len(plan.parts) == 2 and known > 2:
            pair = call(
                bind(stack_kernel), shape((2,) + trial_cols.shape, bf16), [VMEM] * 2
            )(pieces[1], pieces[2])
            for n in (0, known - 1):
                pieces.append(swap(pieces[n], "blk", blks, stride))
            pieces.append(swap(pair, "blk", blks, stride))
            masks += [masks[n] ^ stride for n in (0, known - 1)]
            break
        for d in range(1, radix):
            for n in range(known):
                pieces.append(swap(pieces[n], "blk", blks, d * stride))
                masks.append(masks[n] ^ (d * stride))
        if known == 1:
            pieces[-1] = call(
                bind(copy_kernel), shape(trial_cols.shape, bf16), [VMEM], flops=HEAD
            )(pieces[-1])
    if len(plan.parts) == 2:
        slots = tuple(masks) + (tuple(masks[n] ^ stride for n in (1, 2)),)
    else:
        pieces = [p for _, p in sorted(zip(masks, pieces), key=lambda pair: pair[0])]

    if plan.aligned:
        mine = call(
            after(bind(place_kernel, slots), 0), shape(half, bf16), [VMEM] * (len(pieces) + 1)
        )(vir_values, *pieces)
        other = swap(mine, "vec", vecs, 1)
    else:
        me, vec = lax.axis_index("blk"), lax.axis_index("vec")
        mine = jnp.take(jnp.stack(pieces), me ^ jnp.arange(blks), axis=0)
        both = jnp.stack([mine, swap(mine, "vec", vecs, 1)])
        both = jnp.take(both, vec ^ jnp.arange(vecs), axis=0)
        both = both.transpose(2, 1, 0, 3).reshape(k, vecs, plan.length)
        mine, other = both[None, :, 0], both[None, :, 1]

    flops = k * plan.aux * plan.pairs
    part = call(bind(fac_kernel, 0), shape((k, plan.aux), f32), [VMEM] * 2, flops)(
        mine, coulomb_factors
    )

    cut = (batches + 1) // 2
    spans = [tuple(range(cut)), tuple(range(cut, batches))]
    chunks = [(len(span), k, points) for span in spans]
    grid_flops = 2 * points * virs * occs * k

    def occ_scratch(span):
        return pltpu.VMEM((len(span), plan.occ_all, points), f32)

    first_dens, sent, rows = call(
        after(bind(first_dens_kernel, spans[0]), 4),
        (shape(chunks[0], f32), shape(chunks[0], bf16), shape((occs * k, virs), bf16)),
        [VMEM] * 4 + [ANY],
        grid_flops * len(spans[0]),
        [occ_scratch(spans[0])],
    )(mine, other, vir_values, occ_values, part)
    first_other = swap(sent, "grp", groups, 1)
    second_dens, sent, part = call(
        bind(second_dens_kernel, spans[1]),
        (
            shape(chunks[1], f32),
            shape((len(spans[1]) + plan.slots, k, points), bf16),
            shape((k, plan.aux), f32),
        ),
        [VMEM] * 6,
        grid_flops * len(spans[1]) + flops,
        [occ_scratch(spans[1])],
    )(rows, vir_values, occ_values, other, coulomb_factors, part)
    second_other = swap(sent, "grp", groups, 1)

    def grid(chosen, chunk, dens, came, skip, *more):
        used = plan.run * len(chosen)
        count = 6 + (skip is not None)
        body = bind(grid_kernel, chosen, spans[chunk], skip)
        return call(
            after(body, count) if len(more) + 6 > count else body,
            shape((used * k, virs), f32),
            [SMEM] + [VMEM] * (count - 1) + [ANY] * (len(more) + 6 - count),
            grid_flops * len(spans[chunk]) * used // occs,
            [pltpu.VMEM((used * k, points), bf16), occ_scratch(spans[chunk])],
        )(live_points, dens, came, occ_values, kernel, vir_values, *more)

    every = sum(plan.parts, ())
    begun = grid(every, 0, first_dens, first_other, None, sent)

    def finish(number, *order):
        skip = sum(len(chosen) for chosen in plan.parts[:number]) * plan.run * k
        return grid(plan.parts[number], 1, second_dens, second_other, skip, begun, *order)

    def back(number, acc, *order):
        chosen = plan.parts[number]
        share = (len(plan.masks(chosen)),) + half[1:]
        body = bind(back_kernel, chosen)
        return call(
            after(body, 4) if order else body,
            (shape(share, f32), shape(share, bf16)),
            [VMEM] * 4 + [ANY] * len(order),
            2 * flops // len(plan.parts),
        )(part, second_other, coulomb_factors, acc, *order)

    if len(plan.parts) == 2:
        (stride, radix), (top, _) = digits
        count = plan.count // 2

        def first_sum(stay, sent, *order):
            body = bind(sum_kernel, radix)
            return call(
                after(body, 2) if order else body,
                (shape((count // radix,) + half[1:], f32),)
                + (shape((count // radix,) + half[1:], bf16),) * (radix - 1),
                [VMEM] * 2 + [ANY] * len(order),
            )(stay, swap(sent, "vec", vecs, 1), *order)

        def next_sum(number, own, sends):
            came = [swap(x, "blk", blks, (d + 1) * stride) for d, x in enumerate(sends)]
            out = [shape(half[1:], bf16 if d else f32) for d in plan.parts[number]]
            outs = call(bind(split_kernel), out, [VMEM] * (1 + len(came)))(own, *came)
            return [
                swap(x, "blk", blks, d * top) if d else x
                for d, x in zip(plan.parts[number], outs)
            ]

        stay, sent = back(0, finish(0))
        acc = finish(1, stay)
        far = first_sum(stay, sent, acc)
        stay, sent = back(1, acc, far[0])
        near = first_sum(stay, sent)
        came = next_sum(0, far[0], far[1:]) + next_sum(1, near[0], near[1:])
    else:
        stay, sent = back(0, finish(0))
        full = jnp.concatenate([stay[0], sent[0].astype(f32)], axis=1)
        full = full.reshape(k, blks, vecs, plan.rows).transpose(2, 1, 0, 3)
        full = jnp.take(full, me ^ jnp.arange(blks), axis=1)
        full = jnp.take(full, vec ^ jnp.arange(vecs), axis=0)
        total = full[0] + swap(full[1].astype(bf16), "vec", vecs, 1).astype(f32)
        for stride, radix in digits:
            total = total.reshape((-1, radix) + total.shape[1:])
            total = sum(
                (
                    swap(total[:, d].astype(bf16), "blk", blks, d * stride).astype(f32)
                    for d in range(1, radix)
                ),
                total[:, 0],
            )
        came = [total[0]]
    total = sum((x.astype(f32) for x in came[1:]), came[0].astype(f32))
    result = energy_gap[None, :] * trial_cols.astype(f32) + total
    return result.astype(bf16).T


def solution(mesh):
    sizes = tuple(mesh.shape[a] for a in ("grp", "blk", "vec"))
    in_specs = (
        P(("grp", "blk", "vec"), None),
        P(("grp", "blk", "vec")),
        P("blk", None),
        P("blk", None, None),
        P("blk", None, None),
        P("blk", None),
        P("blk"),
    )
    out_specs = P(("grp", "blk", "vec"), None)

    def program(*args):
        return local(*args, sizes=sizes)

    return jax.shard_map(
        program, mesh=mesh, in_specs=in_specs, out_specs=out_specs, check_vma=False
    )
```

```python
import jax
import jax.numpy as jnp
from jax import lax
from jax.experimental import pallas as pl
from jax.experimental.pallas import tpu as pltpu
from jax.sharding import PartitionSpec as P


LANES = 128
HEAD = 10**10
NT = (((1,), (1,)), ((), ()))
NN = (((1,), (0,)), ((), ()))
VMEM = pl.BlockSpec(memory_space=pltpu.VMEM)
SMEM = pl.BlockSpec(memory_space=pltpu.SMEM)
ANY = pl.BlockSpec(memory_space=pl.ANY)


def digits_of(count):
    digits, stride = [], 1
    bits = count.bit_length() - 1
    if bits % 2:
        digits.append((1, 2))
        stride = 2
    while stride < count:
        digits.append((stride, 4))
        stride *= 4
    return digits


def swap(x, axis, count, mask):
    return lax.ppermute(x, axis, [(i, i ^ mask) for i in range(count)])


def call(body, out_shape, in_specs, flops=0, scratch=(), limit=14):
    return pl.pallas_call(
        body,
        out_shape=out_shape,
        in_specs=in_specs,
        out_specs=jax.tree.map(lambda _: VMEM, out_shape),
        scratch_shapes=list(scratch),
        compiler_params=pltpu.CompilerParams(vmem_limit_bytes=limit * 2**20),
        cost_estimate=pl.CostEstimate(flops=flops, bytes_accessed=0, transcendentals=0),
    )


def after(body, count):
    return lambda *refs: body(*refs[:count], *refs[count + 1 :])


def shape(dims, dtype):
    return jax.ShapeDtypeStruct(dims, dtype)


class Plan:
    def __init__(self, sizes, trial, coulomb_factors, occ_values, vir_values):
        self.groups, self.blks, self.vecs = sizes
        self.rows, self.k = trial.shape
        self.aux = coulomb_factors.shape[0] // self.vecs
        self.pairs = coulomb_factors.shape[1] // self.groups
        self.batches = occ_values.shape[0] // self.vecs
        self.occ_all, self.points = occ_values.shape[1:]
        self.occs = self.occ_all // self.groups
        self.virs = vir_values.shape[2]
        self.aligned = self.rows % LANES == 0
        self.count = self.blks if self.aligned else 1
        self.length = self.rows if self.aligned else self.pairs // self.vecs
        self.per = self.length // LANES
        self.digits = digits_of(self.blks)
        stride, radix = self.digits[-1]
        self.top = stride
        if self.aligned and radix == 4 and len(self.digits) == 2 and self.occs % radix == 0:
            self.parts = [(2, 3), (0, 1)]
            self.run = self.occs // radix
        else:
            assert not self.aligned
            self.parts = [(0,)]
            self.run = self.occs

    def masks(self, part):
        if len(self.parts) == 1:
            return list(range(self.count))
        return [d * self.top + low for d in part for low in range(self.top)]

    def first_row(self, d):
        return (lax.axis_index("blk") // self.top ^ d) * self.run if len(self.parts) > 1 else 0

    def owner(self, m):
        return lax.axis_index("blk") ^ m if self.aligned else 0

    def part(self, h):
        return lax.axis_index("vec") ^ h if self.aligned else h

    def block(self, h, m, j):
        return (self.owner(m) * self.vecs + self.part(h)) * self.per + j

    def place(self, h, m, j):
        at = self.block(h, m, j)
        tiles = self.virs // LANES
        return (
            pl.ds(pl.multiple_of((at // tiles) * self.k, self.k), self.k),
            pl.ds(pl.multiple_of((at % tiles) * LANES, LANES), LANES),
        )


def copy_kernel(plan, given, out):
    out[...] = given[...]


def stack_kernel(plan, *refs):
    for m, piece in enumerate(refs[:-1]):
        refs[-1][m] = piece[...]


def occ_rows(plan, occ, b, occ32):
    occ32[...] = occ[lax.axis_index("vec") * plan.batches + b].astype(jnp.float32)
    base = lax.axis_index("grp") * plan.occs
    return lambda i: occ32[pl.ds(base + i, 1), :]


def factor_block(plan, fac, m, p):
    top = pl.multiple_of(lax.axis_index("vec") * plan.aux, plan.aux)
    at = lax.axis_index("grp") * plan.pairs + (plan.owner(m) * plan.vecs + p) * plan.length
    return fac[pl.ds(top, plan.aux), pl.ds(pl.multiple_of(at, LANES), plan.length)]


def rows_kernel(plan, mine, other, rows):
    for h, half in enumerate((mine, other)):
        for m in range(plan.count):
            for j in range(plan.per):
                rows[plan.place(h, m, j)] = half[m, :, j * LANES : (j + 1) * LANES]


def dens_kernel(plan, span, rows, vir, occ, dens, sent, occ32):
    k = plan.k
    vec = lax.axis_index("vec")
    for n, b in enumerate(span):
        row = occ_rows(plan, occ, b, occ32.at[n])
        trans = lax.dot_general(
            rows[...], vir[vec * plan.batches + b], NT, preferred_element_type=jnp.float32
        )
        total = row(0) * trans[:k, :]
        for i in range(1, plan.occs):
            total = total + row(i) * trans[i * k : (i + 1) * k, :]
        dens[n] = total
        sent[n] = total.astype(sent.dtype)


def first_dens_kernel(plan, span, mine, other, vir, occ, dens, sent, rows, occ32):
    rows_kernel(plan, mine, other, rows)
    dens_kernel(plan, span, rows, vir, occ, dens, sent, occ32)


def fac_kernel(plan, h, half, fac, *refs):
    value = refs[0][...] if len(refs) > 1 else 0.0
    for m in range(plan.count):
        value += lax.dot_general(
            half[m], factor_block(plan, fac, m, plan.part(h)), NT, preferred_element_type=jnp.float32
        )
    refs[-1][...] = value


def grid_kernel(plan, part, span, skip, live, dens_a, dens_b, occ, weight, vir, *refs):
    acc, scaled, occ32 = refs[-3:]
    k = plan.k
    base = lax.axis_index("vec") * plan.batches
    slots = lax.broadcasted_iota(jnp.int32, (1, plan.points), 1)
    for n, b in enumerate(span):
        row = occ_rows(plan, occ, b, occ32.at[n])
        density = dens_a[n] + dens_b[n].astype(jnp.float32)
        used = jnp.where(slots < live[base + b], weight[pl.ds(base + b, 1), :], 0.0)
        weighted = density * used
        for t, d in enumerate(part):
            first = plan.first_row(d)
            for r in range(plan.run):
                at = (t * plan.run + r) * k
                scaled[at : at + k, :] = (row(first + r) * weighted).astype(jnp.bfloat16)
        value = lax.dot_general(scaled[...], vir[base + b], NN, preferred_element_type=jnp.float32)
        if n:
            acc[...] += value
        elif skip is None:
            acc[...] = value
        else:
            acc[...] = refs[0][pl.ds(skip, acc.shape[0]), :] + value


def back_kernel(plan, part, part_a, part_b, fac, acc, stay, sent):
    both = (part_a[...] + part_b[...]).astype(jnp.bfloat16)
    k, tiles = plan.k, plan.virs // LANES
    masks = plan.masks(part)
    for n, m in enumerate(masks):
        t = n * len(part) // len(masks)
        first = plan.first_row(part[t])
        for h, out in enumerate((stay, sent)):
            value = 2.0 * lax.dot_general(
                both,
                factor_block(plan, fac, m, plan.part(h)),
                NN,
                preferred_element_type=jnp.float32,
            )
            for j in range(plan.per):
                at = plan.block(h, m, j)
                row = (at // tiles - first + t * plan.run) * k
                found = acc[
                    pl.ds(pl.multiple_of(row, k), k),
                    pl.ds(pl.multiple_of((at % tiles) * LANES, LANES), LANES),
                ]
                lanes = slice(j * LANES, (j + 1) * LANES)
                out[n, :, lanes] = (value[:, lanes] + found).astype(out.dtype)


def sum_kernel(plan, radix, stay, came, *outs):
    for n in range(stay.shape[0]):
        out = outs[n % radix]
        out[n // radix] = (stay[n] + came[n].astype(jnp.float32)).astype(out.dtype)


def split_kernel(plan, own, *refs):
    outs = refs[-own.shape[0] :]
    for n, out in enumerate(outs):
        total = own[n]
        for came in refs[: -len(outs)]:
            total = total + came[n].astype(jnp.float32)
        out[...] = total.astype(out.dtype)


def local(trial, energy_gap, coulomb_factors, occ_values, vir_values, kernel, live_points, sizes):
    plan = Plan(sizes, trial, coulomb_factors, occ_values, vir_values)
    groups, blks, vecs, k = plan.groups, plan.blks, plan.vecs, plan.k
    batches, points, virs, occs = plan.batches, plan.points, plan.virs, plan.occs
    digits = plan.digits
    half = (plan.count, k, plan.length)
    bf16, f32 = jnp.bfloat16, jnp.float32

    def bind(body, *first):
        return lambda *refs: body(plan, *first, *refs)

    trial_cols = trial.T
    pieces, masks = [trial_cols], [0]
    for stride, radix in reversed(digits):
        known = len(masks)
        for d in range(1, radix):
            for n in range(known):
                pieces.append(swap(pieces[n], "blk", blks, d * stride))
                masks.append(masks[n] ^ (d * stride))
        if known == 1:
            pieces[-1] = call(
                bind(copy_kernel), shape(trial_cols.shape, bf16), [VMEM], flops=HEAD
            )(pieces[-1])
    pieces = [p for _, p in sorted(zip(masks, pieces), key=lambda pair: pair[0])]

    if plan.aligned:
        mine = call(
            after(bind(stack_kernel), 0), shape(half, bf16), [VMEM] * (len(pieces) + 1)
        )(vir_values, *pieces)
        other = swap(mine, "vec", vecs, 1)
    else:
        me, vec = lax.axis_index("blk"), lax.axis_index("vec")
        mine = jnp.take(jnp.stack(pieces), me ^ jnp.arange(blks), axis=0)
        both = jnp.stack([mine, swap(mine, "vec", vecs, 1)])
        both = jnp.take(both, vec ^ jnp.arange(vecs), axis=0)
        both = both.transpose(2, 1, 0, 3).reshape(k, vecs, plan.length)
        mine, other = both[None, :, 0], both[None, :, 1]

    flops = k * plan.aux * plan.pairs
    part = call(bind(fac_kernel, 0), shape((k, plan.aux), f32), [VMEM] * 2, flops)(
        mine, coulomb_factors
    )

    cut = (batches + 1) // 2
    spans = [tuple(range(cut)), tuple(range(cut, batches))]
    chunks = [(len(span), k, points) for span in spans]
    grid_flops = 2 * points * virs * occs * k

    def occ_scratch(span):
        return pltpu.VMEM((len(span), plan.occ_all, points), f32)

    first_dens, sent, rows = call(
        after(bind(first_dens_kernel, spans[0]), 4),
        (shape(chunks[0], f32), shape(chunks[0], bf16), shape((occs * k, virs), bf16)),
        [VMEM] * 4 + [ANY],
        grid_flops * len(spans[0]),
        [occ_scratch(spans[0])],
    )(mine, other, vir_values, occ_values, part)
    first_other = swap(sent, "grp", groups, 1)
    second_dens, sent = call(
        bind(dens_kernel, spans[1]),
        (shape(chunks[1], f32), shape(chunks[1], bf16)),
        [VMEM] * 3,
        grid_flops * len(spans[1]),
        [occ_scratch(spans[1])],
    )(rows, vir_values, occ_values)
    second_other = swap(sent, "grp", groups, 1)
    part = call(
        after(bind(fac_kernel, 1), 2), shape((k, plan.aux), f32), [VMEM] * 2 + [ANY, VMEM], flops
    )(other, coulomb_factors, sent, part)
    other_part = swap(part, "grp", groups, 1)

    def grid(chosen, chunk, dens, came, skip, *more):
        used = plan.run * len(chosen)
        count = 6 + (skip is not None)
        body = bind(grid_kernel, chosen, spans[chunk], skip)
        return call(
            after(body, count) if len(more) + 6 > count else body,
            shape((used * k, virs), f32),
            [SMEM] + [VMEM] * (count - 1) + [ANY] * (len(more) + 6 - count),
            grid_flops * len(spans[chunk]) * used // occs,
            [pltpu.VMEM((used * k, points), bf16), occ_scratch(spans[chunk])],
        )(live_points, dens, came, occ_values, kernel, vir_values, *more)

    every = sum(plan.parts, ())
    begun = grid(every, 0, first_dens, first_other, None, part)

    def finish(number, *order):
        skip = sum(len(chosen) for chosen in plan.parts[:number]) * plan.run * k
        return grid(plan.parts[number], 1, second_dens, second_other, skip, begun, *order)

    def back(number, acc, *order):
        chosen = plan.parts[number]
        share = (len(plan.masks(chosen)),) + half[1:]
        body = bind(back_kernel, chosen)
        return call(
            after(body, 4) if order else body,
            (shape(share, f32), shape(share, bf16)),
            [VMEM] * 4 + [ANY] * len(order),
            2 * flops // len(plan.parts),
        )(part, other_part, coulomb_factors, acc, *order)

    if len(plan.parts) == 2:
        (stride, radix), (top, _) = digits
        count = plan.count // 2

        def first_sum(stay, sent, *order):
            body = bind(sum_kernel, radix)
            return call(
                after(body, 2) if order else body,
                (shape((count // radix,) + half[1:], f32),)
                + (shape((count // radix,) + half[1:], bf16),) * (radix - 1),
                [VMEM] * 2 + [ANY] * len(order),
            )(stay, swap(sent, "vec", vecs, 1), *order)

        def next_sum(number, own, sends):
            came = [swap(x, "blk", blks, (d + 1) * stride) for d, x in enumerate(sends)]
            out = [shape(half[1:], bf16 if d else f32) for d in plan.parts[number]]
            outs = call(bind(split_kernel), out, [VMEM] * (1 + len(came)))(own, *came)
            return [
                swap(x, "blk", blks, d * top) if d else x
                for d, x in zip(plan.parts[number], outs)
            ]

        stay, sent = back(0, finish(0))
        acc = finish(1, stay)
        far = first_sum(stay, sent, acc)
        stay, sent = back(1, acc, far[0])
        near = first_sum(stay, sent)
        came = next_sum(0, far[0], far[1:]) + next_sum(1, near[0], near[1:])
    else:
        stay, sent = back(0, finish(0))
        full = jnp.concatenate([stay[0], sent[0].astype(f32)], axis=1)
        full = full.reshape(k, blks, vecs, plan.rows).transpose(2, 1, 0, 3)
        full = jnp.take(full, me ^ jnp.arange(blks), axis=1)
        full = jnp.take(full, vec ^ jnp.arange(vecs), axis=0)
        total = full[0] + swap(full[1].astype(bf16), "vec", vecs, 1).astype(f32)
        for stride, radix in digits:
            total = total.reshape((-1, radix) + total.shape[1:])
            total = sum(
                (
                    swap(total[:, d].astype(bf16), "blk", blks, d * stride).astype(f32)
                    for d in range(1, radix)
                ),
                total[:, 0],
            )
        came = [total[0]]
    total = sum((x.astype(f32) for x in came[1:]), came[0].astype(f32))
    result = energy_gap[None, :] * trial_cols.astype(f32) + total
    return result.astype(bf16).T


def solution(mesh):
    sizes = tuple(mesh.shape[a] for a in ("grp", "blk", "vec"))
    in_specs = (
        P(("grp", "blk", "vec"), None),
        P(("grp", "blk", "vec")),
        P("blk", None),
        P("blk", None, None),
        P("blk", None, None),
        P("blk", None),
        P("blk"),
    )
    out_specs = P(("grp", "blk", "vec"), None)

    def program(*args):
        return local(*args, sizes=sizes)

    return jax.shard_map(
        program, mesh=mesh, in_specs=in_specs, out_specs=out_specs, check_vma=False
    )
```

```python
import jax
import jax.numpy as jnp
from jax import lax
from jax.experimental import pallas as pl
from jax.experimental.pallas import tpu as pltpu
from jax.sharding import PartitionSpec as P


LANES = 128
HEAD = 10**10
NT = (((1,), (1,)), ((), ()))
NN = (((1,), (0,)), ((), ()))
VMEM = pl.BlockSpec(memory_space=pltpu.VMEM)
SMEM = pl.BlockSpec(memory_space=pltpu.SMEM)
ANY = pl.BlockSpec(memory_space=pl.ANY)


def digits_of(count):
    digits, stride = [], 1
    bits = count.bit_length() - 1
    if bits % 2:
        digits.append((1, 2))
        stride = 2
    while stride < count:
        digits.append((stride, 4))
        stride *= 4
    return digits


def swap(x, axis, count, mask):
    return lax.ppermute(x, axis, [(i, i ^ mask) for i in range(count)])


def call(body, out_shape, in_specs, flops=0, scratch=(), limit=14):
    return pl.pallas_call(
        body,
        out_shape=out_shape,
        in_specs=in_specs,
        out_specs=jax.tree.map(lambda _: VMEM, out_shape),
        scratch_shapes=list(scratch),
        compiler_params=pltpu.CompilerParams(vmem_limit_bytes=limit * 2**20),
        cost_estimate=pl.CostEstimate(flops=flops, bytes_accessed=0, transcendentals=0),
    )


def after(body, count):
    return lambda *refs: body(*refs[:count], *refs[count + 1 :])


def shape(dims, dtype):
    return jax.ShapeDtypeStruct(dims, dtype)


class Plan:
    def __init__(self, sizes, trial, coulomb_factors, occ_values, vir_values):
        self.groups, self.blks, self.vecs = sizes
        self.rows, self.k = trial.shape
        self.aux = coulomb_factors.shape[0] // self.vecs
        self.pairs = coulomb_factors.shape[1] // self.groups
        self.batches = occ_values.shape[0] // self.vecs
        self.occ_all, self.points = occ_values.shape[1:]
        self.occs = self.occ_all // self.groups
        self.virs = vir_values.shape[2]
        self.aligned = self.rows % LANES == 0
        self.count = self.blks if self.aligned else 1
        self.length = self.rows if self.aligned else self.pairs // self.vecs
        self.per = self.length // LANES
        self.digits = digits_of(self.blks)
        stride, radix = self.digits[-1]
        self.top = stride
        if self.aligned and radix == 4 and len(self.digits) == 2 and self.occs % radix == 0:
            self.parts = [(2, 3), (0, 1)]
            self.run = self.occs // radix
        else:
            assert not self.aligned
            self.parts = [(0,)]
            self.run = self.occs

    def masks(self, part):
        if len(self.parts) == 1:
            return list(range(self.count))
        return [d * self.top + low for d in part for low in range(self.top)]

    def first_row(self, d):
        return (lax.axis_index("blk") // self.top ^ d) * self.run if len(self.parts) > 1 else 0

    def owner(self, m):
        return lax.axis_index("blk") ^ m if self.aligned else 0

    def part(self, h):
        return lax.axis_index("vec") ^ h if self.aligned else h

    def block(self, h, m, j):
        return (self.owner(m) * self.vecs + self.part(h)) * self.per + j

    def place(self, h, m, j):
        at = self.block(h, m, j)
        tiles = self.virs // LANES
        return (
            pl.ds(pl.multiple_of((at // tiles) * self.k, self.k), self.k),
            pl.ds(pl.multiple_of((at % tiles) * LANES, LANES), LANES),
        )


def copy_kernel(plan, given, out):
    out[...] = given[...]


def stack_kernel(plan, *refs):
    for m, piece in enumerate(refs[:-1]):
        refs[-1][m] = piece[...]


def occ_rows(plan, occ, b, occ32):
    occ32[...] = occ[lax.axis_index("vec") * plan.batches + b].astype(jnp.float32)
    base = lax.axis_index("grp") * plan.occs
    return lambda i: occ32[pl.ds(base + i, 1), :]


def factor_block(plan, fac, m, p):
    top = pl.multiple_of(lax.axis_index("vec") * plan.aux, plan.aux)
    at = lax.axis_index("grp") * plan.pairs + (plan.owner(m) * plan.vecs + p) * plan.length
    return fac[pl.ds(top, plan.aux), pl.ds(pl.multiple_of(at, LANES), plan.length)]


def rows_kernel(plan, mine, other, rows):
    for h, half in enumerate((mine, other)):
        for m in range(plan.count):
            for j in range(plan.per):
                rows[plan.place(h, m, j)] = half[m, :, j * LANES : (j + 1) * LANES]


def dens_kernel(plan, span, rows, vir, occ, dens, sent, occ32):
    k = plan.k
    vec = lax.axis_index("vec")
    for n, b in enumerate(span):
        row = occ_rows(plan, occ, b, occ32.at[n])
        trans = lax.dot_general(
            rows[...], vir[vec * plan.batches + b], NT, preferred_element_type=jnp.float32
        )
        total = row(0) * trans[:k, :]
        for i in range(1, plan.occs):
            total = total + row(i) * trans[i * k : (i + 1) * k, :]
        dens[n] = total
        sent[n] = total.astype(sent.dtype)


def first_dens_kernel(plan, span, mine, other, vir, occ, dens, sent, rows, occ32):
    rows_kernel(plan, mine, other, rows)
    dens_kernel(plan, span, rows, vir, occ, dens, sent, occ32)


def fac_kernel(plan, h, half, fac, *refs):
    value = refs[0][...] if len(refs) > 1 else 0.0
    for m in range(plan.count):
        value += lax.dot_general(
            half[m], factor_block(plan, fac, m, plan.part(h)), NT, preferred_element_type=jnp.float32
        )
    refs[-1][...] = value


def grid_kernel(plan, part, spans, more, live, *refs):
    pairs = refs[: 2 * len(spans)]
    occ, weight, vir = refs[2 * len(spans) : 2 * len(spans) + 3]
    acc, scaled, occ32 = refs[-3:]
    k = plan.k
    base = lax.axis_index("vec") * plan.batches
    slots = lax.broadcasted_iota(jnp.int32, (1, plan.points), 1)
    begun = more
    for c, span in enumerate(spans):
        for n, b in enumerate(span):
            row = occ_rows(plan, occ, b, occ32.at[b - spans[0][0]])
            density = pairs[2 * c][n] + pairs[2 * c + 1][n].astype(jnp.float32)
            used = jnp.where(slots < live[base + b], weight[pl.ds(base + b, 1), :], 0.0)
            weighted = density * used
            for t, d in enumerate(part):
                first = plan.first_row(d)
                for r in range(plan.run):
                    at = (t * plan.run + r) * k
                    scaled[at : at + k, :] = (row(first + r) * weighted).astype(jnp.bfloat16)
            value = lax.dot_general(
                scaled[...], vir[base + b], NN, preferred_element_type=jnp.float32
            )
            if not begun:
                acc[...] = value
            elif more and c == n == 0:
                acc[...] = refs[2 * len(spans) + 3][...] + value
            else:
                acc[...] += value
            begun = True


def back_kernel(plan, part, part_a, part_b, fac, acc, stay, sent):
    both = (part_a[...] + part_b[...]).astype(jnp.bfloat16)
    k, tiles = plan.k, plan.virs // LANES
    masks = plan.masks(part)
    for n, m in enumerate(masks):
        t = n * len(part) // len(masks)
        first = plan.first_row(part[t])
        for h, out in enumerate((stay, sent)):
            value = 2.0 * lax.dot_general(
                both,
                factor_block(plan, fac, m, plan.part(h)),
                NN,
                preferred_element_type=jnp.float32,
            )
            for j in range(plan.per):
                at = plan.block(h, m, j)
                row = (at // tiles - first + t * plan.run) * k
                found = acc[
                    pl.ds(pl.multiple_of(row, k), k),
                    pl.ds(pl.multiple_of((at % tiles) * LANES, LANES), LANES),
                ]
                lanes = slice(j * LANES, (j + 1) * LANES)
                out[n, :, lanes] = (value[:, lanes] + found).astype(out.dtype)


def sum_kernel(plan, radix, stay, came, *outs):
    for n in range(stay.shape[0]):
        out = outs[n % radix]
        out[n // radix] = (stay[n] + came[n].astype(jnp.float32)).astype(out.dtype)


def split_kernel(plan, own, *refs):
    outs = refs[-own.shape[0] :]
    for n, out in enumerate(outs):
        total = own[n]
        for came in refs[: -len(outs)]:
            total = total + came[n].astype(jnp.float32)
        out[...] = total.astype(out.dtype)


def local(trial, energy_gap, coulomb_factors, occ_values, vir_values, kernel, live_points, sizes):
    plan = Plan(sizes, trial, coulomb_factors, occ_values, vir_values)
    groups, blks, vecs, k = plan.groups, plan.blks, plan.vecs, plan.k
    batches, points, virs, occs = plan.batches, plan.points, plan.virs, plan.occs
    digits = plan.digits
    half = (plan.count, k, plan.length)
    bf16, f32 = jnp.bfloat16, jnp.float32

    def bind(body, *first):
        return lambda *refs: body(plan, *first, *refs)

    trial_cols = trial.T
    pieces, masks = [trial_cols], [0]
    for stride, radix in reversed(digits):
        known = len(masks)
        for d in range(radix - 1, 0, -1):
            for n in range(known):
                pieces.append(swap(pieces[n], "blk", blks, d * stride))
                masks.append(masks[n] ^ (d * stride))
        if known == 1:
            pieces[-1] = call(
                bind(copy_kernel), shape(trial_cols.shape, bf16), [VMEM], flops=HEAD
            )(pieces[-1])
    pieces = [p for _, p in sorted(zip(masks, pieces), key=lambda pair: pair[0])]

    if plan.aligned:
        mine = call(
            after(bind(stack_kernel), 0), shape(half, bf16), [VMEM] * (len(pieces) + 1)
        )(vir_values, *pieces)
        other = swap(mine, "vec", vecs, 1)
    else:
        me, vec = lax.axis_index("blk"), lax.axis_index("vec")
        mine = jnp.take(jnp.stack(pieces), me ^ jnp.arange(blks), axis=0)
        both = jnp.stack([mine, swap(mine, "vec", vecs, 1)])
        both = jnp.take(both, vec ^ jnp.arange(vecs), axis=0)
        both = both.transpose(2, 1, 0, 3).reshape(k, vecs, plan.length)
        mine, other = both[None, :, 0], both[None, :, 1]

    flops = k * plan.aux * plan.pairs
    part = call(bind(fac_kernel, 0), shape((k, plan.aux), f32), [VMEM] * 2, flops)(
        mine, coulomb_factors
    )

    cut = (batches + 1) // 2
    spans = [tuple(range(cut)), tuple(range(cut, batches))]
    chunks = [(len(span), k, points) for span in spans]
    grid_flops = 2 * points * virs * occs * k

    def occ_scratch(span):
        return pltpu.VMEM((len(span), plan.occ_all, points), f32)

    first_dens, sent, rows = call(
        after(bind(first_dens_kernel, spans[0]), 4),
        (shape(chunks[0], f32), shape(chunks[0], bf16), shape((occs * k, virs), bf16)),
        [VMEM] * 4 + [ANY],
        grid_flops * len(spans[0]),
        [occ_scratch(spans[0])],
    )(mine, other, vir_values, occ_values, part)
    first_other = swap(sent, "grp", groups, 1)
    second_dens, sent = call(
        bind(dens_kernel, spans[1]),
        (shape(chunks[1], f32), shape(chunks[1], bf16)),
        [VMEM] * 3,
        grid_flops * len(spans[1]),
        [occ_scratch(spans[1])],
    )(rows, vir_values, occ_values)
    second_other = swap(sent, "grp", groups, 1)
    part = call(
        after(bind(fac_kernel, 1), 2), shape((k, plan.aux), f32), [VMEM] * 2 + [ANY, VMEM], flops
    )(other, coulomb_factors, sent, part)
    other_part = swap(part, "grp", groups, 1)

    density = [(first_dens, first_other), (second_dens, second_other)]

    def grid(number, chunks, begun=(), order=()):
        chosen = plan.parts[number]
        used = plan.run * len(chosen)
        body = bind(grid_kernel, chosen, [spans[c] for c in chunks], len(begun) > 0)
        given = [x for c in chunks for x in density[c]]
        count = 4 + len(given) + len(begun)
        batch = sum(spans[c][-1] + 1 - spans[c][0] for c in chunks)
        return call(
            after(body, count) if order else body,
            shape((used * k, virs), f32),
            [SMEM] + [VMEM] * (count - 1) + [ANY] * len(order),
            grid_flops * batch * used // occs,
            [
                pltpu.VMEM((used * k, points), bf16),
                pltpu.VMEM((batch, plan.occ_all, points), f32),
            ],
        )(live_points, *given, occ_values, kernel, vir_values, *begun, *order)

    def back(number, acc, *order):
        chosen = plan.parts[number]
        share = (len(plan.masks(chosen)),) + half[1:]
        body = bind(back_kernel, chosen)
        return call(
            after(body, 4) if order else body,
            (shape(share, f32), shape(share, bf16)),
            [VMEM] * 4 + [ANY] * len(order),
            2 * flops // len(plan.parts),
        )(part, other_part, coulomb_factors, acc, *order)

    if len(plan.parts) == 2:
        (stride, radix), (top, _) = digits
        count = plan.count // 2

        def first_sum(stay, sent, *order):
            body = bind(sum_kernel, radix)
            return call(
                after(body, 2) if order else body,
                (shape((count // radix,) + half[1:], f32),)
                + (shape((count // radix,) + half[1:], bf16),) * (radix - 1),
                [VMEM] * 2 + [ANY] * len(order),
            )(stay, swap(sent, "vec", vecs, 1), *order)

        def next_sum(number, own, sends):
            came = [swap(x, "blk", blks, (d + 1) * stride) for d, x in enumerate(sends)]
            out = [shape(half[1:], bf16 if d else f32) for d in plan.parts[number]]
            outs = call(bind(split_kernel), out, [VMEM] * (1 + len(came)))(own, *came)
            return [
                swap(x, "blk", blks, d * top) if d else x
                for d, x in zip(plan.parts[number], outs)
            ]

        stay, sent = back(0, grid(0, (1,), (grid(0, (0,), (), (part,)),)))
        acc = grid(1, (0, 1), (), (stay,))
        far = first_sum(stay, sent, acc)
        stay, sent = back(1, acc, far[0])
        near = first_sum(stay, sent)
        came = next_sum(0, far[0], far[1:]) + next_sum(1, near[0], near[1:])
    else:
        stay, sent = back(0, grid(0, (0, 1)))
        full = jnp.concatenate([stay[0], sent[0].astype(f32)], axis=1)
        full = full.reshape(k, blks, vecs, plan.rows).transpose(2, 1, 0, 3)
        full = jnp.take(full, me ^ jnp.arange(blks), axis=1)
        full = jnp.take(full, vec ^ jnp.arange(vecs), axis=0)
        total = full[0] + swap(full[1].astype(bf16), "vec", vecs, 1).astype(f32)
        for stride, radix in digits:
            total = total.reshape((-1, radix) + total.shape[1:])
            total = sum(
                (
                    swap(total[:, d].astype(bf16), "blk", blks, d * stride).astype(f32)
                    for d in range(1, radix)
                ),
                total[:, 0],
            )
        came = [total[0]]
    total = sum((x.astype(f32) for x in came[1:]), came[0].astype(f32))
    result = energy_gap[None, :] * trial_cols.astype(f32) + total
    return result.astype(bf16).T


def solution(mesh):
    sizes = tuple(mesh.shape[a] for a in ("grp", "blk", "vec"))
    in_specs = (
        P(("grp", "blk", "vec"), None),
        P(("grp", "blk", "vec")),
        P("blk", None),
        P("blk", None, None),
        P("blk", None, None),
        P("blk", None),
        P("blk"),
    )
    out_specs = P(("grp", "blk", "vec"), None)

    def program(*args):
        return local(*args, sizes=sizes)

    return jax.shard_map(
        program, mesh=mesh, in_specs=in_specs, out_specs=out_specs, check_vma=False
    )
```

```python
import jax
import jax.numpy as jnp
from jax import lax
from jax.experimental import pallas as pl
from jax.experimental.pallas import tpu as pltpu
from jax.sharding import PartitionSpec as P


LANES = 128
HEAD = 10**10
NT = (((1,), (1,)), ((), ()))
NN = (((1,), (0,)), ((), ()))
VMEM = pl.BlockSpec(memory_space=pltpu.VMEM)
SMEM = pl.BlockSpec(memory_space=pltpu.SMEM)
ANY = pl.BlockSpec(memory_space=pl.ANY)


def digits_of(count):
    digits, stride = [], 1
    bits = count.bit_length() - 1
    if bits % 2:
        digits.append((1, 2))
        stride = 2
    while stride < count:
        digits.append((stride, 4))
        stride *= 4
    return digits


def swap(x, axis, count, mask):
    return lax.ppermute(x, axis, [(i, i ^ mask) for i in range(count)])


def call(body, out_shape, in_specs, flops=0, scratch=(), limit=14):
    return pl.pallas_call(
        body,
        out_shape=out_shape,
        in_specs=in_specs,
        out_specs=jax.tree.map(lambda _: VMEM, out_shape),
        scratch_shapes=list(scratch),
        compiler_params=pltpu.CompilerParams(vmem_limit_bytes=limit * 2**20),
        cost_estimate=pl.CostEstimate(flops=flops, bytes_accessed=0, transcendentals=0),
    )


def after(body, count):
    return lambda *refs: body(*refs[:count], *refs[count + 1 :])


def shape(dims, dtype):
    return jax.ShapeDtypeStruct(dims, dtype)


class Plan:
    def __init__(self, sizes, trial, coulomb_factors, occ_values, vir_values):
        self.groups, self.blks, self.vecs = sizes
        self.rows, self.k = trial.shape
        self.aux = coulomb_factors.shape[0] // self.vecs
        self.pairs = coulomb_factors.shape[1] // self.groups
        self.batches = occ_values.shape[0] // self.vecs
        self.occ_all, self.points = occ_values.shape[1:]
        self.occs = self.occ_all // self.groups
        self.virs = vir_values.shape[2]
        self.aligned = self.rows % LANES == 0
        self.count = self.blks if self.aligned else 1
        self.length = self.rows if self.aligned else self.pairs // self.vecs
        self.per = self.length // LANES
        self.digits = digits_of(self.blks)
        stride, radix = self.digits[-1]
        self.top = stride
        if self.aligned and radix == 4 and len(self.digits) == 2 and self.occs % radix == 0:
            self.parts = [(2, 3), (0, 1)]
            self.run = self.occs // radix
        else:
            assert not self.aligned
            self.parts = [(0,)]
            self.run = self.occs

    def masks(self, part):
        if len(self.parts) == 1:
            return list(range(self.count))
        return [d * self.top + low for d in part for low in range(self.top)]

    def first_row(self, d):
        return (lax.axis_index("blk") // self.top ^ d) * self.run if len(self.parts) > 1 else 0

    def owner(self, m):
        return lax.axis_index("blk") ^ m if self.aligned else 0

    def part(self, h):
        return lax.axis_index("vec") ^ h if self.aligned else h

    def block(self, h, m, j):
        return (self.owner(m) * self.vecs + self.part(h)) * self.per + j

    def place(self, h, m, j):
        at = self.block(h, m, j)
        tiles = self.virs // LANES
        return (
            pl.ds(pl.multiple_of((at // tiles) * self.k, self.k), self.k),
            pl.ds(pl.multiple_of((at % tiles) * LANES, LANES), LANES),
        )


def copy_kernel(plan, given, out):
    out[...] = given[...]


def stack_kernel(plan, *refs):
    for m, piece in enumerate(refs[:-1]):
        refs[-1][m] = piece[...]


def occ_rows(plan, occ, b, occ32):
    occ32[...] = occ[lax.axis_index("vec") * plan.batches + b].astype(jnp.float32)
    base = lax.axis_index("grp") * plan.occs
    return lambda i: occ32[pl.ds(base + i, 1), :]


def factor_block(plan, fac, m, p):
    top = pl.multiple_of(lax.axis_index("vec") * plan.aux, plan.aux)
    at = lax.axis_index("grp") * plan.pairs + (plan.owner(m) * plan.vecs + p) * plan.length
    return fac[pl.ds(top, plan.aux), pl.ds(pl.multiple_of(at, LANES), plan.length)]


def rows_kernel(plan, groups, halves, rows):
    for h, half in enumerate(halves):
        for blocks, ref in zip(groups, half):
            for n, m in enumerate(blocks):
                for j in range(plan.per):
                    rows[plan.place(h, m, j)] = ref[n, :, j * LANES : (j + 1) * LANES]


def dens_kernel(plan, span, rows, vir, occ, dens, sent, occ32):
    k = plan.k
    vec = lax.axis_index("vec")
    for n, b in enumerate(span):
        row = occ_rows(plan, occ, b, occ32.at[n])
        trans = lax.dot_general(
            rows[...], vir[vec * plan.batches + b], NT, preferred_element_type=jnp.float32
        )
        total = row(0) * trans[:k, :]
        for i in range(1, plan.occs):
            total = total + row(i) * trans[i * k : (i + 1) * k, :]
        dens[n] = total
        sent[n] = total.astype(sent.dtype)


def first_dens_kernel(plan, span, groups, *refs):
    count = len(groups)
    vir, occ, dens, sent, rows, occ32 = refs[2 * count :]
    rows_kernel(plan, groups, (refs[:count], refs[count : 2 * count]), rows)
    dens_kernel(plan, span, rows, vir, occ, dens, sent, occ32)


def fac_kernel(plan, h, blocks, half, fac, *refs):
    value = refs[0][...] if len(refs) > 1 else 0.0
    for n, m in enumerate(blocks):
        value += lax.dot_general(
            half[n], factor_block(plan, fac, m, plan.part(h)), NT, preferred_element_type=jnp.float32
        )
    refs[-1][...] = value


def grid_kernel(plan, part, span, skip, live, dens_a, dens_b, occ, weight, vir, *refs):
    acc, scaled, occ32 = refs[-3:]
    k = plan.k
    base = lax.axis_index("vec") * plan.batches
    slots = lax.broadcasted_iota(jnp.int32, (1, plan.points), 1)
    for n, b in enumerate(span):
        row = occ_rows(plan, occ, b, occ32.at[n])
        density = dens_a[n] + dens_b[n].astype(jnp.float32)
        used = jnp.where(slots < live[base + b], weight[pl.ds(base + b, 1), :], 0.0)
        weighted = density * used
        for t, d in enumerate(part):
            first = plan.first_row(d)
            for r in range(plan.run):
                at = (t * plan.run + r) * k
                scaled[at : at + k, :] = (row(first + r) * weighted).astype(jnp.bfloat16)
        value = lax.dot_general(scaled[...], vir[base + b], NN, preferred_element_type=jnp.float32)
        if n:
            acc[...] += value
        elif skip is None:
            acc[...] = value
        else:
            acc[...] = refs[0][pl.ds(skip, acc.shape[0]), :] + value


def back_kernel(plan, part, part_a, part_b, fac, acc, stay, sent):
    both = (part_a[...] + part_b[...]).astype(jnp.bfloat16)
    k, tiles = plan.k, plan.virs // LANES
    masks = plan.masks(part)
    for n, m in enumerate(masks):
        t = n * len(part) // len(masks)
        first = plan.first_row(part[t])
        for h, out in enumerate((stay, sent)):
            value = 2.0 * lax.dot_general(
                both,
                factor_block(plan, fac, m, plan.part(h)),
                NN,
                preferred_element_type=jnp.float32,
            )
            for j in range(plan.per):
                at = plan.block(h, m, j)
                row = (at // tiles - first + t * plan.run) * k
                found = acc[
                    pl.ds(pl.multiple_of(row, k), k),
                    pl.ds(pl.multiple_of((at % tiles) * LANES, LANES), LANES),
                ]
                lanes = slice(j * LANES, (j + 1) * LANES)
                out[n, :, lanes] = (value[:, lanes] + found).astype(out.dtype)


def sum_kernel(plan, radix, stay, came, *outs):
    for n in range(stay.shape[0]):
        out = outs[n % radix]
        out[n // radix] = (stay[n] + came[n].astype(jnp.float32)).astype(out.dtype)


def split_kernel(plan, own, *refs):
    outs = refs[-own.shape[0] :]
    for n, out in enumerate(outs):
        total = own[n]
        for came in refs[: -len(outs)]:
            total = total + came[n].astype(jnp.float32)
        out[...] = total.astype(out.dtype)


def local(trial, energy_gap, coulomb_factors, occ_values, vir_values, kernel, live_points, sizes):
    plan = Plan(sizes, trial, coulomb_factors, occ_values, vir_values)
    groups, blks, vecs, k = plan.groups, plan.blks, plan.vecs, plan.k
    batches, points, virs, occs = plan.batches, plan.points, plan.virs, plan.occs
    digits = plan.digits
    half = (plan.count, k, plan.length)
    bf16, f32 = jnp.bfloat16, jnp.float32

    def bind(body, *first):
        return lambda *refs: body(plan, *first, *refs)

    trial_cols = trial.T
    flops = k * plan.aux * plan.pairs

    def fac_call(h, blocks, half, *more, order=()):
        count = 2 + len(more)
        body = bind(fac_kernel, h, blocks)
        return call(
            after(body, count) if order else body,
            shape((k, plan.aux), f32),
            [VMEM] * count + [ANY] * len(order),
            flops * len(blocks) // plan.count,
        )(half, coulomb_factors, *more, *order)

    pieces, masks = [trial_cols], [0]
    for stride, radix in reversed(digits):
        known = len(masks)
        for d in range(1, radix):
            for n in range(known):
                pieces.append(swap(pieces[n], "blk", blks, d * stride))
                masks.append(masks[n] ^ (d * stride))
        if known == 1:
            pieces[-1] = call(
                bind(copy_kernel), shape(trial_cols.shape, bf16), [VMEM], flops=HEAD
            )(pieces[-1])

    def stack(chosen, *order):
        body = bind(stack_kernel)
        for _ in order:
            body = after(body, 0)
        return call(
            body,
            shape((len(chosen),) + trial_cols.shape, bf16),
            [VMEM] * (len(chosen) + len(order)),
        )(*order, *chosen)

    if len(plan.parts) == 2:
        count = plan.count // 2
        sets = [tuple(masks[:count]), tuple(masks[count:])]
        mine = [stack(pieces[:count], vir_values)]
        other = [swap(mine[0], "vec", vecs, 1)]
        part = fac_call(0, sets[0], mine[0])
        part = fac_call(1, sets[0], other[0], part)
        mine.append(stack(pieces[count:], part))
        other.append(swap(mine[1], "vec", vecs, 1))
        part = fac_call(0, sets[1], mine[1], part)
    else:
        pieces = [p for _, p in sorted(zip(masks, pieces), key=lambda pair: pair[0])]
        me, vec = lax.axis_index("blk"), lax.axis_index("vec")
        mine = jnp.take(jnp.stack(pieces), me ^ jnp.arange(blks), axis=0)
        both = jnp.stack([mine, swap(mine, "vec", vecs, 1)])
        both = jnp.take(both, vec ^ jnp.arange(vecs), axis=0)
        both = both.transpose(2, 1, 0, 3).reshape(k, vecs, plan.length)
        mine, other = [both[None, :, 0]], [both[None, :, 1]]
        sets = [(0,)]
        part = fac_call(0, sets[0], mine[0])

    cut = (batches + 1) // 2
    spans = [tuple(range(cut)), tuple(range(cut, batches))]
    chunks = [(len(span), k, points) for span in spans]
    grid_flops = 2 * points * virs * occs * k

    def occ_scratch(span):
        return pltpu.VMEM((len(span), plan.occ_all, points), f32)

    first_dens, sent, rows = call(
        after(bind(first_dens_kernel, spans[0], sets), 2 * len(sets) + 2),
        (shape(chunks[0], f32), shape(chunks[0], bf16), shape((occs * k, virs), bf16)),
        [VMEM] * (2 * len(sets) + 2) + [ANY],
        grid_flops * len(spans[0]),
        [occ_scratch(spans[0])],
    )(*mine, *other, vir_values, occ_values, part)
    first_other = swap(sent, "grp", groups, 1)
    second_dens, sent = call(
        bind(dens_kernel, spans[1]),
        (shape(chunks[1], f32), shape(chunks[1], bf16)),
        [VMEM] * 3,
        grid_flops * len(spans[1]),
        [occ_scratch(spans[1])],
    )(rows, vir_values, occ_values)
    second_other = swap(sent, "grp", groups, 1)
    part = fac_call(1, sets[-1], other[-1], part, order=(sent,))
    other_part = swap(part, "grp", groups, 1)

    def grid(chosen, chunk, dens, came, skip, *more):
        used = plan.run * len(chosen)
        count = 6 + (skip is not None)
        body = bind(grid_kernel, chosen, spans[chunk], skip)
        return call(
            after(body, count) if len(more) + 6 > count else body,
            shape((used * k, virs), f32),
            [SMEM] + [VMEM] * (count - 1) + [ANY] * (len(more) + 6 - count),
            grid_flops * len(spans[chunk]) * used // occs,
            [pltpu.VMEM((used * k, points), bf16), occ_scratch(spans[chunk])],
        )(live_points, dens, came, occ_values, kernel, vir_values, *more)

    every = sum(plan.parts, ())
    begun = grid(every, 0, first_dens, first_other, None, part)

    def finish(number, *order):
        skip = sum(len(chosen) for chosen in plan.parts[:number]) * plan.run * k
        return grid(plan.parts[number], 1, second_dens, second_other, skip, begun, *order)

    def back(number, acc, *order):
        chosen = plan.parts[number]
        share = (len(plan.masks(chosen)),) + half[1:]
        body = bind(back_kernel, chosen)
        return call(
            after(body, 4) if order else body,
            (shape(share, f32), shape(share, bf16)),
            [VMEM] * 4 + [ANY] * len(order),
            2 * flops // len(plan.parts),
        )(part, other_part, coulomb_factors, acc, *order)

    if len(plan.parts) == 2:
        (stride, radix), (top, _) = digits
        count = plan.count // 2

        def first_sum(stay, sent, *order):
            body = bind(sum_kernel, radix)
            return call(
                after(body, 2) if order else body,
                (shape((count // radix,) + half[1:], f32),)
                + (shape((count // radix,) + half[1:], bf16),) * (radix - 1),
                [VMEM] * 2 + [ANY] * len(order),
            )(stay, swap(sent, "vec", vecs, 1), *order)

        def next_sum(number, own, sends):
            came = [swap(x, "blk", blks, (d + 1) * stride) for d, x in enumerate(sends)]
            out = [shape(half[1:], bf16 if d else f32) for d in plan.parts[number]]
            outs = call(bind(split_kernel), out, [VMEM] * (1 + len(came)))(own, *came)
            return [
                swap(x, "blk", blks, d * top) if d else x
                for d, x in zip(plan.parts[number], outs)
            ]

        stay, sent = back(0, finish(0))
        acc = finish(1, stay)
        far = first_sum(stay, sent, acc)
        stay, sent = back(1, acc, far[0])
        near = first_sum(stay, sent)
        came = next_sum(0, far[0], far[1:]) + next_sum(1, near[0], near[1:])
    else:
        stay, sent = back(0, finish(0))
        full = jnp.concatenate([stay[0], sent[0].astype(f32)], axis=1)
        full = full.reshape(k, blks, vecs, plan.rows).transpose(2, 1, 0, 3)
        full = jnp.take(full, me ^ jnp.arange(blks), axis=1)
        full = jnp.take(full, vec ^ jnp.arange(vecs), axis=0)
        total = full[0] + swap(full[1].astype(bf16), "vec", vecs, 1).astype(f32)
        for stride, radix in digits:
            total = total.reshape((-1, radix) + total.shape[1:])
            total = sum(
                (
                    swap(total[:, d].astype(bf16), "blk", blks, d * stride).astype(f32)
                    for d in range(1, radix)
                ),
                total[:, 0],
            )
        came = [total[0]]
    total = sum((x.astype(f32) for x in came[1:]), came[0].astype(f32))
    result = energy_gap[None, :] * trial_cols.astype(f32) + total
    return result.astype(bf16).T


def solution(mesh):
    sizes = tuple(mesh.shape[a] for a in ("grp", "blk", "vec"))
    in_specs = (
        P(("grp", "blk", "vec"), None),
        P(("grp", "blk", "vec")),
        P("blk", None),
        P("blk", None, None),
        P("blk", None, None),
        P("blk", None),
        P("blk"),
    )
    out_specs = P(("grp", "blk", "vec"), None)

    def program(*args):
        return local(*args, sizes=sizes)

    return jax.shard_map(
        program, mesh=mesh, in_specs=in_specs, out_specs=out_specs, check_vma=False
    )
```
